8 devices in a mesh: fsdp: 8 (over z, y, x, core).
Axes of the slice: x: 2, y: 2, z: 1, core: 2. Of those that a mesh axis runs over, the one named last changes fastest.
Arguments:
- x_saved: bfloat16 [2, 2, 8, 2048, 1024], P(None, None, 'fsdp')
- grad_out: bfloat16 [2, 8, 2048, 1024], P(None, 'fsdp')
- x_next: bfloat16 [2, 8, 2048, 1024], P(None, 'fsdp')
- w_up: bfloat16 [2, 2, 1024, 4096], replicated
- w_down: bfloat16 [2, 2, 4096, 1024], replicated
- acc_up: float32 [2, 2, 1024, 4096], P(None, None, 'fsdp')
- acc_down: float32 [2, 2, 4096, 1024], P(None, None, 'fsdp')
- master_up: float32 [2, 2, 1024, 4096], P(None, None, 'fsdp')
- master_down: float32 [2, 2, 4096, 1024], P(None, None, 'fsdp')
- moment1_up: float32 [2, 2, 1024, 4096], P(None, None, 'fsdp')
- moment1_down: float32 [2, 2, 4096, 1024], P(None, None, 'fsdp')
- moment2_up: float32 [2, 2, 1024, 4096], P(None, None, 'fsdp')
- moment2_down: float32 [2, 2, 4096, 1024], P(None, None, 'fsdp')
Outputs:
- output 1: float32 [2, 2, 1024, 4096], P(None, None, 'fsdp')
- output 2: float32 [2, 2, 4096, 1024], P(None, None, 'fsdp')
- output 3: float32 [2, 2, 1024, 4096], P(None, None, 'fsdp')
- output 4: float32 [2, 2, 4096, 1024], P(None, None, 'fsdp')
- output 5: float32 [2, 2, 1024, 4096], P(None, None, 'fsdp')
- output 6: float32 [2, 2, 4096, 1024], P(None, None, 'fsdp')
- output 7: bfloat16 [2, 8, 2048, 1024], P(None, 'fsdp')
All inputs are finite; a program needn't handle non-finite values.
Results may differ from the reference program's by a relative error of at most 0.00723387.
Values are sent between devices in bfloat16 or wider.
A program may use at most 1 GiB of HBM per device.

```python
import functools
import jax
import jax.numpy as jnp
from jax import lax

D = 1024
FF = 4096
BATCH = 8
SEQ_LEN = 2048
GROUPS = 8
STAGES = 2
LAYERS = 2
MICROBATCHES = 2
ADAM_STEP = 2
TOKENS = BATCH // GROUPS * SEQ_LEN
LEARN_RATE = 0.005
BETA_ONE = 0.9
BETA_TWO = 0.95
ADAM_EPS = 1e-8
WEIGHT_DECAY = 0.1


def setup_inputs(seed: int = 0) -> dict:
    key_list = jax.random.split(jax.random.key(seed), 13)
    row_count = BATCH * SEQ_LEN
    scale_up = 0.3 * row_count ** 0.5
    scale_down = 0.7 * row_count ** 0.5
    tok_shape = (STAGES, BATCH, SEQ_LEN, D)
    up_shape = (STAGES, LAYERS, D, FF)
    down_shape = (STAGES, LAYERS, FF, D)
    x_saved = jax.random.normal(key_list[0], (STAGES, LAYERS, BATCH, SEQ_LEN, D), jnp.float32).astype(jnp.bfloat16)
    grad_out = jax.random.normal(key_list[1], tok_shape, jnp.float32).astype(jnp.bfloat16)
    x_next = jax.random.normal(key_list[2], tok_shape, jnp.float32).astype(jnp.bfloat16)
    w_up = (jax.random.normal(key_list[3], up_shape, jnp.float32) * D ** -0.5).astype(jnp.bfloat16)
    w_down = (jax.random.normal(key_list[4], down_shape, jnp.float32) * FF ** -0.5).astype(jnp.bfloat16)
    acc_up = jax.random.normal(key_list[5], up_shape, jnp.float32) * scale_up
    acc_down = jax.random.normal(key_list[6], down_shape, jnp.float32) * scale_down
    master_up = jax.random.normal(key_list[7], up_shape, jnp.float32) * D ** -0.5
    master_down = jax.random.normal(key_list[8], down_shape, jnp.float32) * FF ** -0.5
    moment1_up = jax.random.normal(key_list[9], up_shape, jnp.float32) * (0.05 * scale_up)
    moment1_down = jax.random.normal(key_list[10], down_shape, jnp.float32) * (0.05 * scale_down)
    moment2_up = jax.random.uniform(key_list[11], up_shape, jnp.float32, 0.02, 0.06) * scale_up ** 2
    moment2_down = jax.random.uniform(key_list[12], down_shape, jnp.float32, 0.02, 0.06) * scale_down ** 2
    return {'x_saved': x_saved, 'grad_out': grad_out, 'x_next': x_next, 'w_up': w_up, 'w_down': w_down, 'acc_up': acc_up, 'acc_down': acc_down, 'master_up': master_up, 'master_down': master_down, 'moment1_up': moment1_up, 'moment1_down': moment1_down, 'moment2_up': moment2_up, 'moment2_down': moment2_down}


def backward_layer(x_in, cotangent, w_one, w_two):
    hidden = jnp.dot(x_in, w_one, preferred_element_type=jnp.float32)
    gelu_out, gelu_vjp = jax.vjp(jax.nn.gelu, hidden)
    gelu_out = gelu_out.astype(jnp.bfloat16)
    grad_act = jnp.dot(cotangent, w_two.T, preferred_element_type=jnp.float32)
    grad_hidden = gelu_vjp(grad_act)[0].astype(jnp.bfloat16)
    part_down = jnp.dot(gelu_out.T, cotangent, preferred_element_type=jnp.float32)
    part_up = jnp.dot(x_in.T, grad_hidden, preferred_element_type=jnp.float32)
    return part_up, part_down, grad_hidden


def stage_grads(x_layers, grad_top, up_stack, down_stack):
    x_blocks = jnp.swapaxes(x_layers.reshape(LAYERS, GROUPS, TOKENS, D), 0, 1)
    grad_blocks = grad_top.reshape(GROUPS, TOKENS, D)

    def scan_body(carry, block_pair):
        sum_up, sum_down = carry
        x_block, cotangent = block_pair
        up_parts = [None] * LAYERS
        down_parts = [None] * LAYERS
        for layer_id in reversed(range(LAYERS)):
            part_up, part_down, grad_hidden = backward_layer(x_block[layer_id], cotangent, up_stack[layer_id], down_stack[layer_id])
            up_parts[layer_id] = part_up
            down_parts[layer_id] = part_down
            if layer_id > 0:
                cotangent = (cotangent.astype(jnp.float32) + jnp.dot(grad_hidden, up_stack[layer_id].T, preferred_element_type=jnp.float32)).astype(jnp.bfloat16)
        return (sum_up + jnp.stack(up_parts), sum_down + jnp.stack(down_parts)), None

    start_sums = (jnp.zeros((LAYERS, D, FF), jnp.float32), jnp.zeros((LAYERS, FF, D), jnp.float32))
    final_sums, scan_rest = lax.scan(scan_body, start_sums, (x_blocks, grad_blocks))
    return final_sums


def adam_update(acc_part, grad_new, master, moment_one, moment_two):
    grad_mean = (acc_part + grad_new) / MICROBATCHES
    moment_one = BETA_ONE * moment_one + (1.0 - BETA_ONE) * grad_mean
    moment_two = BETA_TWO * moment_two + (1.0 - BETA_TWO) * grad_mean * grad_mean
    corr_one = 1.0 - BETA_ONE ** ADAM_STEP
    corr_two = 1.0 - BETA_TWO ** ADAM_STEP
    step_dir = (moment_one / corr_one) / (jnp.sqrt(moment_two / corr_two) + ADAM_EPS)
    master = master - LEARN_RATE * (step_dir + WEIGHT_DECAY * master)
    return master, moment_one, moment_two


def forward_rows(x_rows, up_stack, down_stack):
    for layer_id in range(LAYERS):
        hidden = jnp.dot(x_rows, up_stack[layer_id], preferred_element_type=jnp.float32)
        gelu_out = jax.nn.gelu(hidden).astype(jnp.bfloat16)
        mlp_val = jnp.dot(gelu_out, down_stack[layer_id], preferred_element_type=jnp.float32)
        x_rows = (x_rows.astype(jnp.float32) + mlp_val).astype(jnp.bfloat16)
    return x_rows


def reference(x_saved, grad_out, x_next, w_up, w_down, acc_up, acc_down, master_up, master_down, moment1_up, moment1_down, moment2_up, moment2_down):
    grads_up = []
    grads_down = []
    for stage_id in range(STAGES):
        sum_up, sum_down = stage_grads(x_saved[stage_id], grad_out[stage_id], w_up[stage_id], w_down[stage_id])
        grads_up.append(sum_up)
        grads_down.append(sum_down)
    new_master_up, new_moment1_up, new_moment2_up = adam_update(acc_up, jnp.stack(grads_up), master_up, moment1_up, moment2_up)
    new_master_down, new_moment1_down, new_moment2_down = adam_update(acc_down, jnp.stack(grads_down), master_down, moment1_down, moment2_down)
    new_up = new_master_up.astype(jnp.bfloat16)
    new_down = new_master_down.astype(jnp.bfloat16)
    outs_next = []
    for stage_id in range(STAGES):
        row_blocks = x_next[stage_id].reshape(GROUPS, TOKENS, D)
        moved = lax.map(functools.partial(forward_rows, up_stack=new_up[stage_id], down_stack=new_down[stage_id]), row_blocks)
        outs_next.append(moved.reshape(BATCH, SEQ_LEN, D))
    y_next = jnp.stack(outs_next)
    return (new_master_up, new_master_down, new_moment1_up, new_moment1_down, new_moment2_up, new_moment2_down, y_next)
```

```python
import functools
import math

import jax
import jax.numpy as jnp
from jax import lax
from jax.experimental import pallas as pl
from jax.experimental.pallas import tpu as pltpu
from jax.sharding import PartitionSpec as P


LEARN_RATE = 0.005
BETA_ONE = 0.9
BETA_TWO = 0.95
ADAM_EPS = 1e-8
WEIGHT_DECAY = 0.1
MICROBATCHES = 2
ADAM_STEP = 2
CORR_ONE = 1.0 - BETA_ONE ** ADAM_STEP
CORR_TWO = 1.0 - BETA_TWO ** ADAM_STEP
GELU_C = math.sqrt(2.0 / math.pi)
GELU_K = 0.044715

D = 1024
FF = 4096
TOK = 2048
TM = 512
NB = TOK // TM
HALVES = 2
FC = FF // 2 // HALVES
BW = FC // 4
ROWS = D // 8
DROWS = FF // 8

F32 = jnp.float32
BF16 = jnp.bfloat16

ANY = pl.BlockSpec(memory_space=pl.ANY)


def dot(a, b, ca, cb):
    return lax.dot_general(a, b, (((ca,), (cb,)), ((), ())), preferred_element_type=F32)


def gelu_pair(h):
    hh = h * h
    t = jnp.tanh(h * (GELU_C + (GELU_C * GELU_K) * hh))
    cdf = 0.5 * t + 0.5
    grad = cdf + h * ((0.5 - 0.5 * (t * t)) * (GELU_C + (3.0 * GELU_C * GELU_K) * hh))
    return h * cdf, grad


def gelu(h):
    t = jnp.tanh(h * (GELU_C + (GELU_C * GELU_K) * (h * h)))
    return h * (0.5 * t + 0.5)


def bwd_kernel(stage, layer, half, mode, part, info, *refs):
    it = iter(refs)
    take = lambda k: [next(it) for _ in range(k)]
    xo, xp, do, dp, w_up, w_down = take(6)
    n_extra = {1: 0, 2: 1, 3: 2}[mode]
    extra_own, extra_par = take(n_extra), take(n_extra)
    sums_in = take(2) if part == "par" else None
    if part == "own":
        sums_out = take(2)
    else:
        outs_even, outs_odd = take(4), take(4)
    if mode != 3:
        dxo = next(it) if part != "par" else None
        dxp = next(it) if part != "own" else None
    xb, db, w1s, w2s, acc1, acc2, act, dhs, insem, wsem, ssem = take(11)
    eb, esem = take(2) if n_extra else (None, None)
    dxb, outsem = take(2) if mode != 3 else (None, None)
    i = pl.program_id(0)
    n = 2 * NB if part == "all" else NB
    base = NB if part == "par" else 0
    slot = lax.rem(i, 2)
    me = info[0]
    core = lax.rem(me, 2)
    chip = lax.div(me, 2)

    def in_copies(own, j, slot):
        rows = pl.ds(pl.multiple_of(j * TM, TM), TM)
        xs, ds, es = (xo, do, extra_own) if own else (xp, dp, extra_par)
        out = [pltpu.make_async_copy(xs.at[stage, layer, 0, rows], xb.at[slot], insem.at[0, slot]),
               pltpu.make_async_copy(ds.at[stage, 0, rows], db.at[slot], insem.at[1, slot])]
        for k, e in enumerate(es):
            out.append(pltpu.make_async_copy(e.at[rows], eb.at[k, slot], esem.at[k, slot]))
        return out

    def fetch(j, slot):
        @pl.when(j < NB)
        def _():
            for c in in_copies(True, j, slot):
                c.start()

        @pl.when(j >= NB)
        def _():
            for c in in_copies(False, j - NB, slot):
                c.start()

    def w_copies():
        out = []
        for j in range(4):
            f0 = pl.multiple_of(j * 1024 + core * 512 + half * BW, BW)
            out.append(pltpu.make_async_copy(w_up.at[stage, layer, :, pl.ds(f0, BW)], w1s.at[:, pl.ds(j * BW, BW)], wsem.at[0, j]))
            out.append(pltpu.make_async_copy(w_down.at[stage, layer, pl.ds(f0, BW), :], w2s.at[pl.ds(j * BW, BW), :], wsem.at[1, j]))
        return out

    @pl.when(i == 0)
    def _():
        fetch(base, 0)
        for c in w_copies():
            c.start()
        if part == "par":
            loads = [pltpu.make_async_copy(a, b, ssem.at[k]) for k, (a, b) in enumerate(zip(sums_in, (acc1, acc2)))]
            for c in loads:
                c.start()
            for c in loads:
                c.wait()
        else:
            acc1[...] = jnp.zeros_like(acc1)
            acc2[...] = jnp.zeros_like(acc2)
        for c in w_copies():
            c.wait()

    @pl.when(i + 1 < n)
    def _():
        fetch(base + i + 1, 1 - slot)

    for c in in_copies(True, 0, slot):
        c.wait()

    def dx_copy(own, j, slot):
        rows = pl.ds(pl.multiple_of(j * TM, TM), TM)
        return pltpu.make_async_copy(dxb.at[slot], (dxo if own else dxp).at[rows], outsem.at[slot])

    if mode != 3:
        @pl.when(i >= 2)
        def _():
            dx_copy(part != "par", 0, slot).wait()

    CH = 256
    n_ch = FC // CH
    x = xb[slot]
    dy = db[slot]
    if mode == 3:
        dy = (dy.astype(F32) + (eb[0, slot] + eb[1, slot])).astype(BF16)

    def front(c):
        cs = slice(c * CH, (c + 1) * CH)
        h = dot(x, w1s[:, cs], 1, 0)
        da = dot(dy, w2s[cs, :], 1, 1)
        g, grad = gelu_pair(h)
        act[:, cs] = g.astype(BF16)
        dhs[:, cs] = (da * grad).astype(BF16)

    def back(c):
        cs = slice(c * CH, (c + 1) * CH)
        acc1[:, cs] += dot(x, dhs[:, cs], 0, 0)
        acc2[cs, :] += dot(act[:, cs], dy, 0, 0)

    for c in range(n_ch):
        front(c)
    for c in range(n_ch):
        back(c)
    if mode != 3:
        dx = dot(dhs[...], w1s[...], 1, 1)
        if mode == 2:
            dx = dx + eb[0, slot]
        dxb[slot] = dx
        if part != "par":
            @pl.when(i < NB)
            def _():
                dx_copy(True, i, slot).start()

        if part != "own":
            @pl.when(i + base >= NB)
            def _():
                dx_copy(False, i + base - NB, slot).start()

    @pl.when(i == n - 1)
    def _():
        if part == "own":
            saves = [pltpu.make_async_copy(a, b, ssem.at[k]) for k, (a, b) in enumerate(zip((acc1, acc2), sums_out))]
            for c in saves:
                c.start()
            for c in saves:
                c.wait()
        else:
            for q in range(4):
                dev = jnp.bitwise_xor(me, 2 * q)
                oc = jnp.bitwise_xor(chip, q)
                outs_even[q][0:ROWS, :] = acc1[pl.ds(pl.multiple_of(dev * ROWS, ROWS), ROWS), :].astype(BF16)
                outs_even[q][ROWS:ROWS + BW, :] = acc2[pl.ds(pl.multiple_of(oc * BW, BW), BW), :].astype(BF16)
                dev = jnp.bitwise_xor(me, 2 * q + 1)
                outs_odd[q][...] = acc1[pl.ds(pl.multiple_of(dev * ROWS, ROWS), ROWS), :].astype(BF16)
        if mode != 3:
            dx_copy(part != "par", 0, 0).wait()
            dx_copy(part != "par", 0, 1).wait()


def bwd_call(stage, layer, half, mode, part, info, base_args, extra_own=(), extra_par=(), sums=()):
    sum_shapes = [jax.ShapeDtypeStruct((D, FC), F32), jax.ShapeDtypeStruct((FC, D), F32)]
    if part == "own":
        out_shape, out_specs = list(sum_shapes), [ANY] * 2
    else:
        out_shape = [jax.ShapeDtypeStruct((ROWS + BW, FC), BF16)] * 4 + [jax.ShapeDtypeStruct((ROWS, FC), BF16)] * 4
        out_specs = [pl.BlockSpec((ROWS + BW, FC), lambda i, s: (0, 0))] * 4 + [pl.BlockSpec((ROWS, FC), lambda i, s: (0, 0))] * 4
    scratch = [
        pltpu.VMEM((2, TM, D), BF16), pltpu.VMEM((2, TM, D), BF16),
        pltpu.VMEM((D, FC), BF16), pltpu.VMEM((FC, D), BF16),
        pltpu.VMEM((D, FC), F32), pltpu.VMEM((FC, D), F32),
        pltpu.VMEM((TM, FC), BF16), pltpu.VMEM((TM, FC), BF16),
        pltpu.SemaphoreType.DMA((2, 2)), pltpu.SemaphoreType.DMA((2, 4)), pltpu.SemaphoreType.DMA((2,)),
    ]
    args = list(base_args) + list(extra_own) + list(extra_par) + list(sums)
    n_extra = len(extra_own)
    if n_extra:
        scratch += [pltpu.VMEM((n_extra, 2, TM, D), F32), pltpu.SemaphoreType.DMA((n_extra, 2))]
    n_tok = 2 * TOK if part == "all" else TOK
    if mode != 3:
        k = 2 if part == "all" else 1
        out_shape += [jax.ShapeDtypeStruct((TOK, D), F32)] * k
        out_specs += [ANY] * k
        scratch += [pltpu.VMEM((2, TM, D), F32), pltpu.SemaphoreType.DMA((2,))]
    return pl.pallas_call(
        functools.partial(bwd_kernel, stage, layer, half, mode, part),
        out_shape=out_shape,
        grid_spec=pltpu.PrefetchScalarGridSpec(
            num_scalar_prefetch=1, grid=(n_tok // TM,), in_specs=[ANY] * len(args), out_specs=out_specs, scratch_shapes=scratch),
        compiler_params=pltpu.CompilerParams(dimension_semantics=("arbitrary",), vmem_limit_bytes=60 * 2 ** 20),
        cost_estimate=pl.CostEstimate(flops=2 * (4 if mode == 3 else 5) * n_tok * D * FC, bytes_accessed=n_tok * 10 * 2 ** 10, transcendentals=n_tok * FC),
    )(info, *args)


def adam(grad_new, acc, master, m1, m2):
    g = (acc + grad_new) / MICROBATCHES
    m1 = BETA_ONE * m1 + (1.0 - BETA_ONE) * g
    m2 = BETA_TWO * m2 + (1.0 - BETA_TWO) * g * g
    step_dir = (m1 * (1.0 / CORR_ONE)) / (jnp.sqrt(m2 * (1.0 / CORR_TWO)) + ADAM_EPS)
    master = master - LEARN_RATE * (step_dir + WEIGHT_DECAY * master)
    return master, m1, m2


def adam_kernel(n_alias, info, *refs):
    up = refs[:16]
    down = refs[16:24]
    au, mu, m1u, m2u, ad, md, m1d, m2d = refs[24:32]
    omu, om1u, om2u, omd, om1d, om2d, w_out = refs[32 + n_alias:]
    core = lax.rem(info[0], 2)
    j = pl.program_id(0)
    up_rows = pl.ds(pl.multiple_of(j * ROWS, ROWS), ROWS)
    for half in range(HALVES):
        for g in range(2):
            total = None
            for q in range(4):
                v = up[half * 8 + 2 * q + g][...].astype(F32)
                total = v if total is None else total + v
            col = jnp.bitwise_xor(core, g) * 512 + half * BW
            cs = pl.ds(pl.multiple_of(col, BW), BW)
            new = adam(total, au[0, 0, :, cs], mu[0, 0, :, cs], m1u[0, 0, :, cs], m2u[0, 0, :, cs])
            omu[0, 0, :, cs] = new[0]
            om1u[0, 0, :, cs] = new[1]
            om2u[0, 0, :, cs] = new[2]
            w_out[up_rows, cs] = new[0].astype(BF16)
        total = None
        for q in range(4):
            v = down[half * 4 + q][...].astype(F32)
            total = v if total is None else total + v
        new = adam(total, ad[0, 0, half], md[0, 0, half], m1d[0, 0, half], m2d[0, 0, half])
        omd[0, 0, half] = new[0]
        om1d[0, 0, half] = new[1]
        om2d[0, 0, half] = new[2]
        w_out[pl.ds(pl.multiple_of(DROWS + half * BW + j * (BW // 4), BW // 4), BW // 4), :] = new[0].astype(BF16)


def adam_call(stage, layer, info, recv, states, prev):
    nj = 4
    dr = BW // nj
    up_spec = pl.BlockSpec((ROWS, BW), lambda j, s: (0, j))
    down_spec = pl.BlockSpec((dr, D), lambda j, s: (ROWS // dr + j, 0))
    st_up = pl.BlockSpec((1, 1, ROWS, FF // nj), lambda j, s: (stage, layer, 0, j))
    st_down = pl.BlockSpec((1, 1, HALVES, dr, D), lambda j, s: (stage, layer, 0, j, 0))
    args, specs = [], []
    for half in range(HALVES):
        for r in range(8):
            args.append(recv[half][r])
            specs.append(up_spec)
    for half in range(HALVES):
        for q in range(4):
            args.append(recv[half][2 * q])
            specs.append(down_spec)
    args += list(states)
    specs += [st_up] * 4 + [st_down] * 4
    n_alias = len(prev)
    args += list(prev)
    specs += [ANY] * n_alias
    up_shape = jax.ShapeDtypeStruct(states[0].shape, F32)
    down_shape = jax.ShapeDtypeStruct(states[4].shape, F32)
    n_in = 1 + len(args) - n_alias
    return pl.pallas_call(
        functools.partial(adam_kernel, n_alias),
        out_shape=[up_shape] * 3 + [down_shape] * 3 + [jax.ShapeDtypeStruct((2 * DROWS, D), BF16)],
        grid_spec=pltpu.PrefetchScalarGridSpec(
            num_scalar_prefetch=1, grid=(nj,), in_specs=specs,
            out_specs=[st_up] * 3 + [st_down] * 3 + [pl.BlockSpec((2 * DROWS, D), lambda j, s: (0, 0))]),
        input_output_aliases={n_in + k: k for k in range(n_alias)},
        compiler_params=pltpu.CompilerParams(dimension_semantics=("arbitrary",), vmem_limit_bytes=60 * 2 ** 20),
        cost_estimate=pl.CostEstimate(flops=20 * 2 ** 20 * 40, bytes_accessed=40 * 2 ** 20, transcendentals=2 ** 20),
    )(info, *args)


def fwd_kernel(has_alias, *refs):
    x_ref, w = refs[:2]
    o_ref, w1s, w2s, sem = refs[2 + has_alias:]
    i = pl.program_id(0)
    CH = DROWS
    n_ch = FF // CH

    def copies(c):
        out = []
        for d in range(8):
            src = w.at[pl.ds(2 * DROWS * d + (c // 2) * ROWS, ROWS), pl.ds((c % 2) * CH, CH)]
            out.append(pltpu.make_async_copy(src, w1s.at[pl.ds(d * ROWS, ROWS), pl.ds(c * CH, CH)], sem.at[0, c]))
        out.append(pltpu.make_async_copy(w.at[pl.ds(2 * DROWS * c + DROWS, CH), :], w2s.at[pl.ds(c * CH, CH), :], sem.at[1, c]))
        return out

    def run(wait):
        x = x_ref[...].reshape(TM, D)
        acc = None
        for c in range(n_ch):
            if wait:
                for cp in copies(c):
                    cp.wait()
            cs = pl.ds(c * CH, CH)
            a = gelu(dot(x, w1s[:, cs], 1, 0)).astype(BF16)
            part = dot(a, w2s[cs, :], 1, 0)
            acc = part if acc is None else acc + part
        o_ref[...] = (x.astype(F32) + acc).astype(BF16).reshape(o_ref.shape)

    @pl.when(i == 0)
    def _():
        for c in range(n_ch):
            for cp in copies(c):
                cp.start()
        run(True)

    @pl.when(i > 0)
    def _():
        run(False)


def fwd_call(stage, layer, x, w, y_prev):
    if layer == 0:
        x_spec = pl.BlockSpec((1, 1, TM, D), lambda i: (stage, 0, i, 0))
        out_shape = jax.ShapeDtypeStruct((TOK, D), BF16)
        o_spec = pl.BlockSpec((TM, D), lambda i: (i, 0))
    else:
        x_spec = pl.BlockSpec((TM, D), lambda i: (i, 0))
        out_shape = jax.ShapeDtypeStruct((2, 1, TOK, D), BF16)
        o_spec = pl.BlockSpec((1, 1, TM, D), lambda i: (stage, 0, i, 0))
    args = [x, w]
    specs = [x_spec, ANY]
    aliases = {}
    if y_prev is not None:
        args.append(y_prev)
        specs.append(ANY)
        aliases = {2: 0}
    return pl.pallas_call(
        functools.partial(fwd_kernel, len(args) - 2),
        out_shape=out_shape,
        grid_spec=pltpu.PrefetchScalarGridSpec(
            num_scalar_prefetch=0, grid=(NB,), in_specs=specs, out_specs=o_spec,
            scratch_shapes=[pltpu.VMEM((D, FF), BF16), pltpu.VMEM((FF, D), BF16), pltpu.SemaphoreType.DMA((2, FF // DROWS))]),
        input_output_aliases=aliases,
        compiler_params=pltpu.CompilerParams(dimension_semantics=("arbitrary",), vmem_limit_bytes=60 * 2 ** 20),
        cost_estimate=pl.CostEstimate(flops=4 * TOK * D * FF, bytes_accessed=26 * 2 ** 20, transcendentals=TOK * FF),
    )(*args)


SEQ = ("bwd_010a", "bwd_010b", "bwd_011", "bwd_110", "adam_01", "bwd_000", "bwd_111", "bwd_001", "bwd_100", "adam_00", "bwd_101", "adam_11", "fwd_00", "adam_10", "fwd_01", "fwd_10", "fwd_11")


def solution(mesh):
    tok_spec = P(None, 'fsdp')
    layer_spec = P(None, None, 'fsdp')
    n_dev = mesh.shape['fsdp']

    def swap(a, r):
        return lax.ppermute(a, 'fsdp', [(d, d ^ r) for d in range(n_dev)])

    def gather(a):
        return lax.all_gather(a, 'fsdp', axis=0, tiled=True)

    def device_step(x_saved, grad_out, x_next, w_up, w_down, acc_up, acc_down, master_up, master_down, moment1_up, moment1_down, moment2_up, moment2_down):
        me = lax.axis_index('fsdp').astype(jnp.int32)
        info = me.reshape(1)

        g_par = swap(grad_out, 1)
        x_par = swap(x_saved, 1)
        base_own = (x_saved, x_saved, grad_out, grad_out, w_up, w_down)
        base = (x_saved, x_par, grad_out, g_par, w_up, w_down)

        down5 = lambda a: a.reshape(2, 2, HALVES, BW, D)
        states = (acc_up, master_up, moment1_up, moment2_up, down5(acc_down), down5(master_down), down5(moment1_down), down5(moment2_down))

        recv = {}
        dx = {}
        outs6 = ()
        full = {}
        hid = {}
        y = None

        for name in SEQ:
            s, l = int(name.split("_")[1][0]), int(name.split("_")[1][1])
            if name.startswith("adam"):
                res = adam_call(s, l, info, recv[s, l], states, outs6)
                outs6 = tuple(res[:6])
                full[s, l] = gather(res[6])
                continue
            if name.startswith("fwd"):
                if l == 0:
                    hid[s] = fwd_call(s, 0, x_next, full[s, 0], None)
                else:
                    y = fwd_call(s, 1, hid[s], full[s, 1], y)
                continue
            half = int(name[6])
            if name == "bwd_010a":
                sum1, sum2, dx_own = bwd_call(s, l, half, 1, "own", info, base_own)
                continue
            if name == "bwd_010b":
                outs = bwd_call(s, l, half, 1, "par", info, base, sums=(sum1, sum2))
                dx[s] = (dx_own, outs[8])
            elif l == 0:
                (own, par), (got_own, got_par) = dx[s]
                outs = bwd_call(s, l, half, 3, "all", info, base, (own, got_own), (par, got_par))
            elif half == 0:
                outs = bwd_call(s, l, half, 1, "all", info, base)
                dx[s] = tuple(outs[8:])
            else:
                own, par = dx[s]
                outs = bwd_call(s, l, half, 2, "all", info, base, (own,), (par,))
                own, par = outs[8:]
                dx[s] = ((own, par), (swap(par, 1), swap(own, 1)))
            msgs = [outs[0], outs[4], outs[1], outs[5], outs[2], outs[6], outs[3], outs[7]]
            recv.setdefault((s, l), []).append([msgs[0]] + [swap(msgs[r], r) for r in range(1, 8)])

        up4 = lambda a: a.reshape(2, 2, DROWS, D)
        return (outs6[0], up4(outs6[3]), outs6[1], up4(outs6[4]), outs6[2], up4(outs6[5]), y)

    return jax.shard_map(device_step, mesh=mesh, in_specs=(layer_spec, tok_spec, tok_spec, P(), P()) + (layer_spec,) * 8, out_specs=(layer_spec,) * 6 + (tok_spec,), check_vma=False)
```

```python
import functools
import math

import jax
import jax.numpy as jnp
from jax import lax
from jax.experimental import pallas as pl
from jax.experimental.pallas import tpu as pltpu
from jax.sharding import PartitionSpec as P


LEARN_RATE = 0.005
BETA_ONE = 0.9
BETA_TWO = 0.95
ADAM_EPS = 1e-8
WEIGHT_DECAY = 0.1
MICROBATCHES = 2
ADAM_STEP = 2
CORR_ONE = 1.0 - BETA_ONE ** ADAM_STEP
CORR_TWO = 1.0 - BETA_TWO ** ADAM_STEP
GELU_C = math.sqrt(2.0 / math.pi)
GELU_K = 0.044715

D = 1024
FF = 4096
TOK = 2048
TM = 512
NB = TOK // TM
HALVES = 2
FC = FF // 2 // HALVES
BW = FC // 4
ROWS = D // 8
DROWS = FF // 8

F32 = jnp.float32
BF16 = jnp.bfloat16

ANY = pl.BlockSpec(memory_space=pl.ANY)


def dot(a, b, ca, cb):
    return lax.dot_general(a, b, (((ca,), (cb,)), ((), ())), preferred_element_type=F32)


def gelu_pair(h):
    hh = h * h
    t = jnp.tanh(h * (GELU_C + (GELU_C * GELU_K) * hh))
    cdf = 0.5 * t + 0.5
    grad = cdf + h * ((0.5 - 0.5 * (t * t)) * (GELU_C + (3.0 * GELU_C * GELU_K) * hh))
    return h * cdf, grad


def gelu(h):
    t = jnp.tanh(h * (GELU_C + (GELU_C * GELU_K) * (h * h)))
    return h * (0.5 * t + 0.5)


def bwd_kernel(stage, layer, half, mode, part, info, *refs):
    it = iter(refs)
    take = lambda k: [next(it) for _ in range(k)]
    xo, xp, do, dp, w_up, w_down = take(6)
    n_extra = {1: 0, 3: 2}[mode]
    extra_own, extra_par = take(n_extra), take(n_extra)
    sums_in = take(2) if part == "par" else None
    if part == "own":
        sums_out = take(2)
    else:
        outs_even, outs_odd = take(4), take(4)
    if mode != 3:
        dho = next(it) if part != "par" else None
        dhp = next(it) if part != "own" else None
    xb, db, w1s, w2s, acc1, acc2, act, dhs, insem, wsem, ssem = take(11)
    eb, esem = take(2) if n_extra else (None, None)
    outsem = next(it) if mode != 3 else None
    i = pl.program_id(0)
    n = 2 * NB if part == "all" else NB
    base = NB if part == "par" else 0
    slot = lax.rem(i, 2)
    me = info[0]
    core = lax.rem(me, 2)
    chip = lax.div(me, 2)

    def in_copies(own, j, slot):
        rows = pl.ds(pl.multiple_of(j * TM, TM), TM)
        xs, ds, es = (xo, do, extra_own) if own else (xp, dp, extra_par)
        out = [pltpu.make_async_copy(xs.at[stage, layer, 0, rows], xb.at[slot], insem.at[0, slot]),
               pltpu.make_async_copy(ds.at[stage, 0, rows], db.at[slot], insem.at[1, slot])]
        for k, e in enumerate(es):
            out.append(pltpu.make_async_copy(e.at[rows], eb.at[k, slot], esem.at[k, slot]))
        return out

    def fetch(j, slot):
        @pl.when(j < NB)
        def _():
            for c in in_copies(True, j, slot):
                c.start()

        @pl.when(j >= NB)
        def _():
            for c in in_copies(False, j - NB, slot):
                c.start()

    def w_copies():
        out = []
        for j in range(4):
            f0 = pl.multiple_of(j * 1024 + core * 512 + half * BW, BW)
            out.append(pltpu.make_async_copy(w_up.at[stage, layer, :, pl.ds(f0, BW)], w1s.at[:, pl.ds(j * BW, BW)], wsem.at[0, j]))
            out.append(pltpu.make_async_copy(w_down.at[stage, layer, pl.ds(f0, BW), :], w2s.at[pl.ds(j * BW, BW), :], wsem.at[1, j]))
        return out

    @pl.when(i == 0)
    def _():
        fetch(base, 0)
        for c in w_copies():
            c.start()
        if part == "par":
            loads = [pltpu.make_async_copy(a, b, ssem.at[k]) for k, (a, b) in enumerate(zip(sums_in, (acc1, acc2)))]
            for c in loads:
                c.start()
            for c in loads:
                c.wait()
        else:
            acc1[...] = jnp.zeros_like(acc1)
            acc2[...] = jnp.zeros_like(acc2)
        for c in w_copies():
            c.wait()

    @pl.when(i + 1 < n)
    def _():
        fetch(base + i + 1, 1 - slot)

    for c in in_copies(True, 0, slot):
        c.wait()

    def dh_copy(own, j, slot):
        rows = pl.ds(pl.multiple_of(j * TM, TM), TM)
        return pltpu.make_async_copy(dhs.at[slot], (dho if own else dhp).at[rows], outsem.at[slot])

    if mode != 3:
        @pl.when(i >= 2)
        def _():
            dh_copy(part != "par", 0, slot).wait()

    CH = 256
    n_ch = FC // CH
    x = xb[slot]
    dy = db[slot]
    if mode == 3:
        dy = (dy.astype(F32) + (eb[0, slot] + eb[1, slot])).astype(BF16)

    def front(c):
        cs = slice(c * CH, (c + 1) * CH)
        h = dot(x, w1s[:, cs], 1, 0)
        da = dot(dy, w2s[cs, :], 1, 1)
        g, grad = gelu_pair(h)
        act[:, cs] = g.astype(BF16)
        dhs[slot, :, cs] = (da * grad).astype(BF16)

    def back(c):
        cs = slice(c * CH, (c + 1) * CH)
        acc1[:, cs] += dot(x, dhs[slot, :, cs], 0, 0)
        acc2[cs, :] += dot(act[:, cs], dy, 0, 0)

    for c in range(n_ch):
        front(c)
    for c in range(n_ch):
        back(c)
    if mode != 3:
        if part != "par":
            @pl.when(i < NB)
            def _():
                dh_copy(True, i, slot).start()

        if part != "own":
            @pl.when(i + base >= NB)
            def _():
                dh_copy(False, i + base - NB, slot).start()

    @pl.when(i == n - 1)
    def _():
        if part == "own":
            saves = [pltpu.make_async_copy(a, b, ssem.at[k]) for k, (a, b) in enumerate(zip((acc1, acc2), sums_out))]
            for c in saves:
                c.start()
            for c in saves:
                c.wait()
        else:
            for q in range(4):
                dev = jnp.bitwise_xor(me, 2 * q)
                oc = jnp.bitwise_xor(chip, q)
                outs_even[q][0:ROWS, :] = acc1[pl.ds(pl.multiple_of(dev * ROWS, ROWS), ROWS), :].astype(BF16)
                outs_even[q][ROWS:ROWS + BW, :] = acc2[pl.ds(pl.multiple_of(oc * BW, BW), BW), :].astype(BF16)
                dev = jnp.bitwise_xor(me, 2 * q + 1)
                outs_odd[q][...] = acc1[pl.ds(pl.multiple_of(dev * ROWS, ROWS), ROWS), :].astype(BF16)
        if mode != 3:
            dh_copy(part != "par", 0, 0).wait()
            dh_copy(part != "par", 0, 1).wait()


def bwd_call(stage, layer, half, mode, part, info, base_args, extra_own=(), extra_par=(), sums=()):
    sum_shapes = [jax.ShapeDtypeStruct((D, FC), F32), jax.ShapeDtypeStruct((FC, D), F32)]
    if part == "own":
        out_shape, out_specs = list(sum_shapes), [ANY] * 2
    else:
        out_shape = [jax.ShapeDtypeStruct((ROWS + BW, FC), BF16)] * 4 + [jax.ShapeDtypeStruct((ROWS, FC), BF16)] * 4
        out_specs = [pl.BlockSpec((ROWS + BW, FC), lambda i, s: (0, 0))] * 4 + [pl.BlockSpec((ROWS, FC), lambda i, s: (0, 0))] * 4
    scratch = [
        pltpu.VMEM((2, TM, D), BF16), pltpu.VMEM((2, TM, D), BF16),
        pltpu.VMEM((D, FC), BF16), pltpu.VMEM((FC, D), BF16),
        pltpu.VMEM((D, FC), F32), pltpu.VMEM((FC, D), F32),
        pltpu.VMEM((TM, FC), BF16), pltpu.VMEM((2, TM, FC), BF16),
        pltpu.SemaphoreType.DMA((2, 2)), pltpu.SemaphoreType.DMA((2, 4)), pltpu.SemaphoreType.DMA((2,)),
    ]
    args = list(base_args) + list(extra_own) + list(extra_par) + list(sums)
    n_extra = len(extra_own)
    if n_extra:
        scratch += [pltpu.VMEM((n_extra, 2, TM, D), F32), pltpu.SemaphoreType.DMA((n_extra, 2))]
    n_tok = 2 * TOK if part == "all" else TOK
    if mode != 3:
        k = 2 if part == "all" else 1
        out_shape += [jax.ShapeDtypeStruct((TOK, FC), BF16)] * k
        out_specs += [ANY] * k
        scratch += [pltpu.SemaphoreType.DMA((2,))]
    return pl.pallas_call(
        functools.partial(bwd_kernel, stage, layer, half, mode, part),
        out_shape=out_shape,
        grid_spec=pltpu.PrefetchScalarGridSpec(
            num_scalar_prefetch=1, grid=(n_tok // TM,), in_specs=[ANY] * len(args), out_specs=out_specs, scratch_shapes=scratch),
        compiler_params=pltpu.CompilerParams(dimension_semantics=("arbitrary",), vmem_limit_bytes=60 * 2 ** 20),
        cost_estimate=pl.CostEstimate(flops=8 * n_tok * D * FC, bytes_accessed=n_tok * 10 * 2 ** 10, transcendentals=n_tok * FC),
    )(info, *args)


def dx_kernel(stage, layer, info, h0o, h0p, h1o, h1p, w_up, dxo, dxp, dhb, w1s, dxb, insem, wsem, outsem):
    i = pl.program_id(0)
    n = 2 * NB
    slot = lax.rem(i, 2)
    core = lax.rem(info[0], 2)

    def in_copies(own, j, slot):
        rows = pl.ds(pl.multiple_of(j * TM, TM), TM)
        pair = (h0o, h1o) if own else (h0p, h1p)
        return [pltpu.make_async_copy(a.at[rows], dhb.at[slot, :, pl.ds(k * FC, FC)], insem.at[k, slot]) for k, a in enumerate(pair)]

    def fetch(j, slot):
        @pl.when(j < NB)
        def _():
            for c in in_copies(False, j, slot):
                c.start()

        @pl.when(j >= NB)
        def _():
            for c in in_copies(True, j - NB, slot):
                c.start()

    def w_copies():
        out = []
        for half in range(HALVES):
            for j in range(4):
                f0 = pl.multiple_of(j * 1024 + core * 512 + half * BW, BW)
                out.append(pltpu.make_async_copy(w_up.at[stage, layer, :, pl.ds(f0, BW)], w1s.at[:, pl.ds(half * FC + j * BW, BW)], wsem.at[half, j]))
        return out

    def out_copy(own, j, slot):
        rows = pl.ds(pl.multiple_of(j * TM, TM), TM)
        return pltpu.make_async_copy(dxb.at[slot], (dxo if own else dxp).at[rows], outsem.at[slot])

    @pl.when(i == 0)
    def _():
        fetch(0, 0)
        for c in w_copies():
            c.start()
        for c in w_copies():
            c.wait()

    @pl.when(i + 1 < n)
    def _():
        fetch(i + 1, 1 - slot)

    for c in in_copies(True, 0, slot):
        c.wait()

    @pl.when(i >= 2)
    def _():
        out_copy(True, 0, slot).wait()

    dxb[slot] = dot(dhb[slot], w1s[...], 1, 1)

    @pl.when(i < NB)
    def _():
        out_copy(False, i, slot).start()

    @pl.when(i >= NB)
    def _():
        out_copy(True, i - NB, slot).start()

    @pl.when(i == n - 1)
    def _():
        out_copy(True, 0, 0).wait()
        out_copy(True, 0, 1).wait()


def dx_call(stage, layer, info, dh0, dh1, w_up):
    args = [dh0[0], dh0[1], dh1[0], dh1[1], w_up]
    return pl.pallas_call(
        functools.partial(dx_kernel, stage, layer),
        out_shape=[jax.ShapeDtypeStruct((TOK, D), F32)] * 2,
        grid_spec=pltpu.PrefetchScalarGridSpec(
            num_scalar_prefetch=1, grid=(2 * NB,), in_specs=[ANY] * 5, out_specs=[ANY] * 2,
            scratch_shapes=[pltpu.VMEM((2, TM, HALVES * FC), BF16), pltpu.VMEM((D, HALVES * FC), BF16), pltpu.VMEM((2, TM, D), F32),
                            pltpu.SemaphoreType.DMA((2, 2)), pltpu.SemaphoreType.DMA((2, 4)), pltpu.SemaphoreType.DMA((2,))]),
        compiler_params=pltpu.CompilerParams(dimension_semantics=("arbitrary",), vmem_limit_bytes=60 * 2 ** 20),
        cost_estimate=pl.CostEstimate(flops=4 * TOK * D * HALVES * FC, bytes_accessed=38 * 2 ** 20, transcendentals=0),
    )(info, *args)


def adam(grad_new, acc, master, m1, m2):
    g = (acc + grad_new) / MICROBATCHES
    m1 = BETA_ONE * m1 + (1.0 - BETA_ONE) * g
    m2 = BETA_TWO * m2 + (1.0 - BETA_TWO) * g * g
    step_dir = (m1 * (1.0 / CORR_ONE)) / (jnp.sqrt(m2 * (1.0 / CORR_TWO)) + ADAM_EPS)
    master = master - LEARN_RATE * (step_dir + WEIGHT_DECAY * master)
    return master, m1, m2


def adam_kernel(n_alias, info, *refs):
    up = refs[:16]
    down = refs[16:24]
    au, mu, m1u, m2u, ad, md, m1d, m2d = refs[24:32]
    omu, om1u, om2u, omd, om1d, om2d, w_out = refs[32 + n_alias:]
    core = lax.rem(info[0], 2)
    j = pl.program_id(0)
    up_rows = pl.ds(pl.multiple_of(j * ROWS, ROWS), ROWS)
    for half in range(HALVES):
        for g in range(2):
            total = None
            for q in range(4):
                v = up[half * 8 + 2 * q + g][...].astype(F32)
                total = v if total is None else total + v
            col = jnp.bitwise_xor(core, g) * 512 + half * BW
            cs = pl.ds(pl.multiple_of(col, BW), BW)
            new = adam(total, au[0, 0, :, cs], mu[0, 0, :, cs], m1u[0, 0, :, cs], m2u[0, 0, :, cs])
            omu[0, 0, :, cs] = new[0]
            om1u[0, 0, :, cs] = new[1]
            om2u[0, 0, :, cs] = new[2]
            w_out[up_rows, cs] = new[0].astype(BF16)
        total = None
        for q in range(4):
            v = down[half * 4 + q][...].astype(F32)
            total = v if total is None else total + v
        new = adam(total, ad[0, 0, half], md[0, 0, half], m1d[0, 0, half], m2d[0, 0, half])
        omd[0, 0, half] = new[0]
        om1d[0, 0, half] = new[1]
        om2d[0, 0, half] = new[2]
        w_out[pl.ds(pl.multiple_of(DROWS + half * BW + j * (BW // 4), BW // 4), BW // 4), :] = new[0].astype(BF16)


def adam_call(stage, layer, info, recv, states, prev):
    nj = 4
    dr = BW // nj
    up_spec = pl.BlockSpec((ROWS, BW), lambda j, s: (0, j))
    down_spec = pl.BlockSpec((dr, D), lambda j, s: (ROWS // dr + j, 0))
    st_up = pl.BlockSpec((1, 1, ROWS, FF // nj), lambda j, s: (stage, layer, 0, j))
    st_down = pl.BlockSpec((1, 1, HALVES, dr, D), lambda j, s: (stage, layer, 0, j, 0))
    args, specs = [], []
    for half in range(HALVES):
        for r in range(8):
            args.append(recv[half][r])
            specs.append(up_spec)
    for half in range(HALVES):
        for q in range(4):
            args.append(recv[half][2 * q])
            specs.append(down_spec)
    args += list(states)
    specs += [st_up] * 4 + [st_down] * 4
    n_alias = len(prev)
    args += list(prev)
    specs += [ANY] * n_alias
    up_shape = jax.ShapeDtypeStruct(states[0].shape, F32)
    down_shape = jax.ShapeDtypeStruct(states[4].shape, F32)
    n_in = 1 + len(args) - n_alias
    return pl.pallas_call(
        functools.partial(adam_kernel, n_alias),
        out_shape=[up_shape] * 3 + [down_shape] * 3 + [jax.ShapeDtypeStruct((2 * DROWS, D), BF16)],
        grid_spec=pltpu.PrefetchScalarGridSpec(
            num_scalar_prefetch=1, grid=(nj,), in_specs=specs,
            out_specs=[st_up] * 3 + [st_down] * 3 + [pl.BlockSpec((2 * DROWS, D), lambda j, s: (0, 0))]),
        input_output_aliases={n_in + k: k for k in range(n_alias)},
        compiler_params=pltpu.CompilerParams(dimension_semantics=("arbitrary",), vmem_limit_bytes=60 * 2 ** 20),
        cost_estimate=pl.CostEstimate(flops=20 * 2 ** 20 * 40, bytes_accessed=40 * 2 ** 20, transcendentals=2 ** 20),
    )(info, *args)


def fwd_kernel(has_alias, *refs):
    x_ref, w = refs[:2]
    o_ref, w1s, w2s, sem = refs[2 + has_alias:]
    i = pl.program_id(0)
    CH = DROWS
    n_ch = FF // CH

    def copies(c):
        out = []
        for d in range(8):
            src = w.at[pl.ds(2 * DROWS * d + (c // 2) * ROWS, ROWS), pl.ds((c % 2) * CH, CH)]
            out.append(pltpu.make_async_copy(src, w1s.at[pl.ds(d * ROWS, ROWS), pl.ds(c * CH, CH)], sem.at[0, c]))
        out.append(pltpu.make_async_copy(w.at[pl.ds(2 * DROWS * c + DROWS, CH), :], w2s.at[pl.ds(c * CH, CH), :], sem.at[1, c]))
        return out

    def run(wait):
        x = x_ref[...].reshape(TM, D)
        acc = None
        for c in range(n_ch):
            if wait:
                for cp in copies(c):
                    cp.wait()
            cs = pl.ds(c * CH, CH)
            a = gelu(dot(x, w1s[:, cs], 1, 0)).astype(BF16)
            part = dot(a, w2s[cs, :], 1, 0)
            acc = part if acc is None else acc + part
        o_ref[...] = (x.astype(F32) + acc).astype(BF16).reshape(o_ref.shape)

    @pl.when(i == 0)
    def _():
        for c in range(n_ch):
            for cp in copies(c):
                cp.start()
        run(True)

    @pl.when(i > 0)
    def _():
        run(False)


def fwd_call(stage, layer, x, w, y_prev):
    if layer == 0:
        x_spec = pl.BlockSpec((1, 1, TM, D), lambda i: (stage, 0, i, 0))
        out_shape = jax.ShapeDtypeStruct((TOK, D), BF16)
        o_spec = pl.BlockSpec((TM, D), lambda i: (i, 0))
    else:
        x_spec = pl.BlockSpec((TM, D), lambda i: (i, 0))
        out_shape = jax.ShapeDtypeStruct((2, 1, TOK, D), BF16)
        o_spec = pl.BlockSpec((1, 1, TM, D), lambda i: (stage, 0, i, 0))
    args = [x, w]
    specs = [x_spec, ANY]
    aliases = {}
    if y_prev is not None:
        args.append(y_prev)
        specs.append(ANY)
        aliases = {2: 0}
    return pl.pallas_call(
        functools.partial(fwd_kernel, len(args) - 2),
        out_shape=out_shape,
        grid_spec=pltpu.PrefetchScalarGridSpec(
            num_scalar_prefetch=0, grid=(NB,), in_specs=specs, out_specs=o_spec,
            scratch_shapes=[pltpu.VMEM((D, FF), BF16), pltpu.VMEM((FF, D), BF16), pltpu.SemaphoreType.DMA((2, FF // DROWS))]),
        input_output_aliases=aliases,
        compiler_params=pltpu.CompilerParams(dimension_semantics=("arbitrary",), vmem_limit_bytes=60 * 2 ** 20),
        cost_estimate=pl.CostEstimate(flops=4 * TOK * D * FF, bytes_accessed=26 * 2 ** 20, transcendentals=TOK * FF),
    )(*args)


SEQ = ("bwd_010a", "bwd_010b", "bwd_011", "bwd_110", "adam_01", "dx_01", "bwd_111", "bwd_000", "dx_11", "bwd_001", "bwd_100", "adam_00", "bwd_101", "adam_11", "adam_10", "fwd_00", "fwd_01", "fwd_10", "fwd_11")


def solution(mesh):
    tok_spec = P(None, 'fsdp')
    layer_spec = P(None, None, 'fsdp')
    n_dev = mesh.shape['fsdp']

    def swap(a, r):
        return lax.ppermute(a, 'fsdp', [(d, d ^ r) for d in range(n_dev)])

    def gather(a):
        return lax.all_gather(a, 'fsdp', axis=0, tiled=True)

    def device_step(x_saved, grad_out, x_next, w_up, w_down, acc_up, acc_down, master_up, master_down, moment1_up, moment1_down, moment2_up, moment2_down):
        me = lax.axis_index('fsdp').astype(jnp.int32)
        info = me.reshape(1)

        g_par = swap(grad_out, 1)
        x_par = swap(x_saved, 1)
        base_own = (x_saved, x_saved, grad_out, grad_out, w_up, w_down)
        base = (x_saved, x_par, grad_out, g_par, w_up, w_down)

        down5 = lambda a: a.reshape(2, 2, HALVES, BW, D)
        states = (acc_up, master_up, moment1_up, moment2_up, down5(acc_down), down5(master_down), down5(moment1_down), down5(moment2_down))

        recv = {}
        dx = {}
        dh = {}
        outs6 = ()
        full = {}
        w_new = {}
        hid = {}
        y = None

        for name in SEQ:
            s, l = int(name.split("_")[1][0]), int(name.split("_")[1][1])
            if name.startswith("adam"):
                res = adam_call(s, l, info, recv[s, l], states, outs6)
                outs6 = tuple(res[:6])
                w_new[s, l] = res[6]
                if (s, l) != (1, 1):
                    full[s, l] = gather(res[6])
                if (s, l) == (1, 0):
                    full[1, 1] = gather(lax.optimization_barrier((w_new[1, 1], res[6]))[0])
                continue
            if name.startswith("fwd"):
                if l == 0:
                    hid[s] = fwd_call(s, 0, x_next, full[s, 0], None)
                else:
                    y = fwd_call(s, 1, hid[s], full[s, 1], y)
                continue
            if name.startswith("dx"):
                own, par = dx_call(s, l, info, dh[s, 0], dh[s, 1], w_up)
                dx[s] = ((own, swap(par, 1)), (par, swap(own, 1)))
                continue
            half = int(name[6])
            if name == "bwd_010a":
                sum1, sum2, dh_own = bwd_call(s, l, half, 1, "own", info, base_own)
                continue
            if name == "bwd_010b":
                outs = bwd_call(s, l, half, 1, "par", info, base, sums=(sum1, sum2))
                dh[s, half] = (dh_own, outs[8])
            elif l == 0:
                outs = bwd_call(s, l, half, 3, "all", info, base, *dx[s])
            else:
                outs = bwd_call(s, l, half, 1, "all", info, base)
                dh[s, half] = tuple(outs[8:])
            msgs = [outs[0], outs[4], outs[1], outs[5], outs[2], outs[6], outs[3], outs[7]]
            recv.setdefault((s, l), []).append([msgs[0]] + [swap(msgs[r], r) for r in range(1, 8)])

        up4 = lambda a: a.reshape(2, 2, DROWS, D)
        return (outs6[0], up4(outs6[3]), outs6[1], up4(outs6[4]), outs6[2], up4(outs6[5]), y)

    return jax.shard_map(device_step, mesh=mesh, in_specs=(layer_spec, tok_spec, tok_spec, P(), P()) + (layer_spec,) * 8, out_specs=(layer_spec,) * 6 + (tok_spec,), check_vma=False)
```

```python
import functools
import math

import jax
import jax.numpy as jnp
from jax import lax
from jax.experimental import pallas as pl
from jax.experimental.pallas import tpu as pltpu
from jax.sharding import PartitionSpec as P


LEARN_RATE = 0.005
BETA_ONE = 0.9
BETA_TWO = 0.95
ADAM_EPS = 1e-8
WEIGHT_DECAY = 0.1
MICROBATCHES = 2
ADAM_STEP = 2
CORR_ONE = 1.0 - BETA_ONE ** ADAM_STEP
CORR_TWO = 1.0 - BETA_TWO ** ADAM_STEP
GELU_C = math.sqrt(2.0 / math.pi)
GELU_K = 0.044715

D = 1024
FF = 4096
TOK = 2048
TM = 512
NB = TOK // TM
HALVES = 2
FC = FF // 2 // HALVES
BW = FC // 4
ROWS = D // 8
DROWS = FF // 8

F32 = jnp.float32
BF16 = jnp.bfloat16

ANY = pl.BlockSpec(memory_space=pl.ANY)


def dot(a, b, ca, cb):
    return lax.dot_general(a, b, (((ca,), (cb,)), ((), ())), preferred_element_type=F32)


def gelu_pair(h):
    hh = h * h
    t = jnp.tanh(h * (GELU_C + (GELU_C * GELU_K) * hh))
    cdf = 0.5 * t + 0.5
    grad = cdf + h * ((0.5 - 0.5 * (t * t)) * (GELU_C + (3.0 * GELU_C * GELU_K) * hh))
    return h * cdf, grad


def gelu(h):
    t = jnp.tanh(h * (GELU_C + (GELU_C * GELU_K) * (h * h)))
    return h * (0.5 * t + 0.5)


def bwd_kernel(stage, layer, half, mode, part, info, *refs):
    it = iter(refs)
    take = lambda k: [next(it) for _ in range(k)]
    xo, xp, do, dp, w_up, w_down = take(6)
    n_extra = {1: 0, 3: 2}[mode]
    extra_own, extra_par = take(n_extra), take(n_extra)
    sums_in = take(2) if part == "par" else None
    if part == "own":
        sums_out = take(2)
    else:
        outs_even, outs_odd = take(4), take(4)
    if mode != 3:
        dho = next(it) if part != "par" else None
        dhp = next(it) if part != "own" else None
    xb, db, w1s, w2s, acc1, acc2, act, dhs, insem, wsem, ssem = take(11)
    eb, esem = take(2) if n_extra else (None, None)
    outsem = next(it) if mode != 3 else None
    i = pl.program_id(0)
    n = 2 * NB if part == "all" else NB
    base = NB if part == "par" else 0
    slot = lax.rem(i, 2)
    me = info[0]
    core = lax.rem(me, 2)
    chip = lax.div(me, 2)

    def in_copies(own, j, slot):
        rows = pl.ds(pl.multiple_of(j * TM, TM), TM)
        xs, ds, es = (xo, do, extra_own) if own else (xp, dp, extra_par)
        out = [pltpu.make_async_copy(xs.at[stage, layer, 0, rows], xb.at[slot], insem.at[0, slot]),
               pltpu.make_async_copy(ds.at[stage, 0, rows], db.at[slot], insem.at[1, slot])]
        for k, e in enumerate(es):
            out.append(pltpu.make_async_copy(e.at[rows], eb.at[k, slot], esem.at[k, slot]))
        return out

    def fetch(j, slot):
        @pl.when(j < NB)
        def _():
            for c in in_copies(True, j, slot):
                c.start()

        @pl.when(j >= NB)
        def _():
            for c in in_copies(False, j - NB, slot):
                c.start()

    def w_copies():
        out = []
        for j in range(4):
            f0 = pl.multiple_of(j * 1024 + core * 512 + half * BW, BW)
            out.append(pltpu.make_async_copy(w_up.at[stage, layer, :, pl.ds(f0, BW)], w1s.at[:, pl.ds(j * BW, BW)], wsem.at[0, j]))
            out.append(pltpu.make_async_copy(w_down.at[stage, layer, pl.ds(f0, BW), :], w2s.at[pl.ds(j * BW, BW), :], wsem.at[1, j]))
        return out

    @pl.when(i == 0)
    def _():
        fetch(base, 0)
        for c in w_copies():
            c.start()
        if part == "par":
            loads = [pltpu.make_async_copy(a, b, ssem.at[k]) for k, (a, b) in enumerate(zip(sums_in, (acc1, acc2)))]
            for c in loads:
                c.start()
            for c in loads:
                c.wait()
        else:
            acc1[...] = jnp.zeros_like(acc1)
            acc2[...] = jnp.zeros_like(acc2)
        for c in w_copies():
            c.wait()

    @pl.when(i + 1 < n)
    def _():
        fetch(base + i + 1, 1 - slot)

    for c in in_copies(True, 0, slot):
        c.wait()

    def dh_copy(own, j, slot):
        rows = pl.ds(pl.multiple_of(j * TM, TM), TM)
        return pltpu.make_async_copy(dhs.at[slot], (dho if own else dhp).at[rows], outsem.at[slot])

    if mode != 3:
        @pl.when(i >= 2)
        def _():
            dh_copy(part != "par", 0, slot).wait()

    CH = 256
    n_ch = FC // CH
    x = xb[slot]
    dy = db[slot]
    if mode == 3:
        dy = (dy.astype(F32) + (eb[0, slot] + eb[1, slot])).astype(BF16)

    def front(c):
        cs = slice(c * CH, (c + 1) * CH)
        h = dot(x, w1s[:, cs], 1, 0)
        da = dot(dy, w2s[cs, :], 1, 1)
        g, grad = gelu_pair(h)
        act[:, cs] = g.astype(BF16)
        dhs[slot, :, cs] = (da * grad).astype(BF16)

    def back(c):
        cs = slice(c * CH, (c + 1) * CH)
        acc1[:, cs] += dot(x, dhs[slot, :, cs], 0, 0)
        acc2[cs, :] += dot(act[:, cs], dy, 0, 0)

    for c in range(n_ch):
        front(c)
    for c in range(n_ch):
        back(c)
    if mode != 3:
        if part != "par":
            @pl.when(i < NB)
            def _():
                dh_copy(True, i, slot).start()

        if part != "own":
            @pl.when(i + base >= NB)
            def _():
                dh_copy(False, i + base - NB, slot).start()

    @pl.when(i == n - 1)
    def _():
        if part == "own":
            saves = [pltpu.make_async_copy(a, b, ssem.at[k]) for k, (a, b) in enumerate(zip((acc1, acc2), sums_out))]
            for c in saves:
                c.start()
            for c in saves:
                c.wait()
        else:
            for q in range(4):
                dev = jnp.bitwise_xor(me, 2 * q)
                oc = jnp.bitwise_xor(chip, q)
                outs_even[q][0:ROWS, :] = acc1[pl.ds(pl.multiple_of(dev * ROWS, ROWS), ROWS), :].astype(BF16)
                outs_even[q][ROWS:ROWS + BW, :] = acc2[pl.ds(pl.multiple_of(oc * BW, BW), BW), :].astype(BF16)
                dev = jnp.bitwise_xor(me, 2 * q + 1)
                outs_odd[q][...] = acc1[pl.ds(pl.multiple_of(dev * ROWS, ROWS), ROWS), :].astype(BF16)
        if mode != 3:
            dh_copy(part != "par", 0, 0).wait()
            dh_copy(part != "par", 0, 1).wait()


def bwd_call(stage, layer, half, mode, part, info, base_args, extra_own=(), extra_par=(), sums=()):
    sum_shapes = [jax.ShapeDtypeStruct((D, FC), F32), jax.ShapeDtypeStruct((FC, D), F32)]
    if part == "own":
        out_shape, out_specs = list(sum_shapes), [ANY] * 2
    else:
        out_shape = [jax.ShapeDtypeStruct((ROWS + BW, FC), BF16)] * 4 + [jax.ShapeDtypeStruct((ROWS, FC), BF16)] * 4
        out_specs = [pl.BlockSpec((ROWS + BW, FC), lambda i, s: (0, 0))] * 4 + [pl.BlockSpec((ROWS, FC), lambda i, s: (0, 0))] * 4
    scratch = [
        pltpu.VMEM((2, TM, D), BF16), pltpu.VMEM((2, TM, D), BF16),
        pltpu.VMEM((D, FC), BF16), pltpu.VMEM((FC, D), BF16),
        pltpu.VMEM((D, FC), F32), pltpu.VMEM((FC, D), F32),
        pltpu.VMEM((TM, FC), BF16), pltpu.VMEM((2, TM, FC), BF16),
        pltpu.SemaphoreType.DMA((2, 2)), pltpu.SemaphoreType.DMA((2, 4)), pltpu.SemaphoreType.DMA((2,)),
    ]
    args = list(base_args) + list(extra_own) + list(extra_par) + list(sums)
    n_extra = len(extra_own)
    if n_extra:
        scratch += [pltpu.VMEM((n_extra, 2, TM, D), F32), pltpu.SemaphoreType.DMA((n_extra, 2))]
    n_tok = 2 * TOK if part == "all" else TOK
    if mode != 3:
        k = 2 if part == "all" else 1
        out_shape += [jax.ShapeDtypeStruct((TOK, FC), BF16)] * k
        out_specs += [ANY] * k
        scratch += [pltpu.SemaphoreType.DMA((2,))]
    return pl.pallas_call(
        functools.partial(bwd_kernel, stage, layer, half, mode, part),
        out_shape=out_shape,
        grid_spec=pltpu.PrefetchScalarGridSpec(
            num_scalar_prefetch=1, grid=(n_tok // TM,), in_specs=[ANY] * len(args), out_specs=out_specs, scratch_shapes=scratch),
        compiler_params=pltpu.CompilerParams(dimension_semantics=("arbitrary",), vmem_limit_bytes=60 * 2 ** 20),
        cost_estimate=pl.CostEstimate(flops=8 * n_tok * D * FC, bytes_accessed=n_tok * 10 * 2 ** 10, transcendentals=n_tok * FC),
    )(info, *args)


def dx_kernel(stage, layer, info, h0o, h0p, h1o, h1p, w_up, dxo, dxp, dhb, w1s, dxb, insem, wsem, outsem):
    i = pl.program_id(0)
    n = 2 * NB
    slot = lax.rem(i, 2)
    core = lax.rem(info[0], 2)

    def in_copies(own, j, slot):
        rows = pl.ds(pl.multiple_of(j * TM, TM), TM)
        pair = (h0o, h1o) if own else (h0p, h1p)
        return [pltpu.make_async_copy(a.at[rows], dhb.at[slot, :, pl.ds(k * FC, FC)], insem.at[k, slot]) for k, a in enumerate(pair)]

    def fetch(j, slot):
        @pl.when(j < NB)
        def _():
            for c in in_copies(False, j, slot):
                c.start()

        @pl.when(j >= NB)
        def _():
            for c in in_copies(True, j - NB, slot):
                c.start()

    def w_copies():
        out = []
        for half in range(HALVES):
            for j in range(4):
                f0 = pl.multiple_of(j * 1024 + core * 512 + half * BW, BW)
                out.append(pltpu.make_async_copy(w_up.at[stage, layer, :, pl.ds(f0, BW)], w1s.at[:, pl.ds(half * FC + j * BW, BW)], wsem.at[half, j]))
        return out

    def out_copy(own, j, slot):
        rows = pl.ds(pl.multiple_of(j * TM, TM), TM)
        return pltpu.make_async_copy(dxb.at[slot], (dxo if own else dxp).at[rows], outsem.at[slot])

    @pl.when(i == 0)
    def _():
        fetch(0, 0)
        for c in w_copies():
            c.start()
        for c in w_copies():
            c.wait()

    @pl.when(i + 1 < n)
    def _():
        fetch(i + 1, 1 - slot)

    for c in in_copies(True, 0, slot):
        c.wait()

    @pl.when(i >= 2)
    def _():
        out_copy(True, 0, slot).wait()

    dxb[slot] = dot(dhb[slot], w1s[...], 1, 1)

    @pl.when(i < NB)
    def _():
        out_copy(False, i, slot).start()

    @pl.when(i >= NB)
    def _():
        out_copy(True, i - NB, slot).start()

    @pl.when(i == n - 1)
    def _():
        out_copy(True, 0, 0).wait()
        out_copy(True, 0, 1).wait()


def dx_call(stage, layer, info, dh0, dh1, w_up):
    args = [dh0[0], dh0[1], dh1[0], dh1[1], w_up]
    return pl.pallas_call(
        functools.partial(dx_kernel, stage, layer),
        out_shape=[jax.ShapeDtypeStruct((TOK, D), F32)] * 2,
        grid_spec=pltpu.PrefetchScalarGridSpec(
            num_scalar_prefetch=1, grid=(2 * NB,), in_specs=[ANY] * 5, out_specs=[ANY] * 2,
            scratch_shapes=[pltpu.VMEM((2, TM, HALVES * FC), BF16), pltpu.VMEM((D, HALVES * FC), BF16), pltpu.VMEM((2, TM, D), F32),
                            pltpu.SemaphoreType.DMA((2, 2)), pltpu.SemaphoreType.DMA((2, 4)), pltpu.SemaphoreType.DMA((2,))]),
        compiler_params=pltpu.CompilerParams(dimension_semantics=("arbitrary",), vmem_limit_bytes=60 * 2 ** 20),
        cost_estimate=pl.CostEstimate(flops=4 * TOK * D * HALVES * FC, bytes_accessed=38 * 2 ** 20, transcendentals=0),
    )(info, *args)


def adam(grad_new, acc, master, m1, m2):
    g = (acc + grad_new) / MICROBATCHES
    m1 = BETA_ONE * m1 + (1.0 - BETA_ONE) * g
    m2 = BETA_TWO * m2 + (1.0 - BETA_TWO) * g * g
    step_dir = (m1 * (1.0 / CORR_ONE)) / (jnp.sqrt(m2 * (1.0 / CORR_TWO)) + ADAM_EPS)
    master = master - LEARN_RATE * (step_dir + WEIGHT_DECAY * master)
    return master, m1, m2


def adam_kernel(n_alias, split, info, *refs):
    up = refs[:16]
    down = refs[16:24]
    au, mu, m1u, m2u, ad, md, m1d, m2d = refs[24:32]
    omu, om1u, om2u, omd, om1d, om2d = refs[32 + n_alias:38 + n_alias]
    w_up_out, w_down_out = refs[38 + n_alias], refs[-1]
    down0 = 0 if split else DROWS
    core = lax.rem(info[0], 2)
    j = pl.program_id(0)
    up_rows = pl.ds(pl.multiple_of(j * ROWS, ROWS), ROWS)
    for half in range(HALVES):
        for g in range(2):
            total = None
            for q in range(4):
                v = up[half * 8 + 2 * q + g][...].astype(F32)
                total = v if total is None else total + v
            col = jnp.bitwise_xor(core, g) * 512 + half * BW
            cs = pl.ds(pl.multiple_of(col, BW), BW)
            new = adam(total, au[0, 0, :, cs], mu[0, 0, :, cs], m1u[0, 0, :, cs], m2u[0, 0, :, cs])
            omu[0, 0, :, cs] = new[0]
            om1u[0, 0, :, cs] = new[1]
            om2u[0, 0, :, cs] = new[2]
            w_up_out[up_rows, cs] = new[0].astype(BF16)
        total = None
        for q in range(4):
            v = down[half * 4 + q][...].astype(F32)
            total = v if total is None else total + v
        new = adam(total, ad[0, 0, half], md[0, 0, half], m1d[0, 0, half], m2d[0, 0, half])
        omd[0, 0, half] = new[0]
        om1d[0, 0, half] = new[1]
        om2d[0, 0, half] = new[2]
        w_down_out[pl.ds(pl.multiple_of(down0 + half * BW + j * (BW // 4), BW // 4), BW // 4), :] = new[0].astype(BF16)


def adam_call(stage, layer, info, recv, states, prev, split):
    nj = 4
    dr = BW // nj
    up_spec = pl.BlockSpec((ROWS, BW), lambda j, s: (0, j))
    down_spec = pl.BlockSpec((dr, D), lambda j, s: (ROWS // dr + j, 0))
    st_up = pl.BlockSpec((1, 1, ROWS, FF // nj), lambda j, s: (stage, layer, 0, j))
    st_down = pl.BlockSpec((1, 1, HALVES, dr, D), lambda j, s: (stage, layer, 0, j, 0))
    args, specs = [], []
    for half in range(HALVES):
        for r in range(8):
            args.append(recv[half][r])
            specs.append(up_spec)
    for half in range(HALVES):
        for q in range(4):
            args.append(recv[half][2 * q])
            specs.append(down_spec)
    args += list(states)
    specs += [st_up] * 4 + [st_down] * 4
    n_alias = len(prev)
    args += list(prev)
    specs += [ANY] * n_alias
    up_shape = jax.ShapeDtypeStruct(states[0].shape, F32)
    down_shape = jax.ShapeDtypeStruct(states[4].shape, F32)
    n_in = 1 + len(args) - n_alias
    w_shapes = [jax.ShapeDtypeStruct((DROWS, D), BF16)] * 2 if split else [jax.ShapeDtypeStruct((2 * DROWS, D), BF16)]
    return pl.pallas_call(
        functools.partial(adam_kernel, n_alias, split),
        out_shape=[up_shape] * 3 + [down_shape] * 3 + w_shapes,
        grid_spec=pltpu.PrefetchScalarGridSpec(
            num_scalar_prefetch=1, grid=(nj,), in_specs=specs,
            out_specs=[st_up] * 3 + [st_down] * 3 + [pl.BlockSpec(w.shape, lambda j, s: (0, 0)) for w in w_shapes]),
        input_output_aliases={n_in + k: k for k in range(n_alias)},
        compiler_params=pltpu.CompilerParams(dimension_semantics=("arbitrary",), vmem_limit_bytes=60 * 2 ** 20),
        cost_estimate=pl.CostEstimate(flops=20 * 2 ** 20 * 40, bytes_accessed=40 * 2 ** 20, transcendentals=2 ** 20),
    )(info, *args)


def fwd_kernel(has_alias, split, *refs):
    x_ref, wu, wd = refs[0], refs[1], refs[1 + split]
    o_ref, w1s, w2s, sem = refs[2 + split + has_alias:]
    per_dev = DROWS if split else 2 * DROWS
    i = pl.program_id(0)
    CH = DROWS
    n_ch = FF // CH

    def copies(c):
        out = []
        for d in range(8):
            src = wu.at[pl.ds(per_dev * d + (c // 2) * ROWS, ROWS), pl.ds((c % 2) * CH, CH)]
            out.append(pltpu.make_async_copy(src, w1s.at[pl.ds(d * ROWS, ROWS), pl.ds(c * CH, CH)], sem.at[0, c]))
        out.append(pltpu.make_async_copy(wd.at[pl.ds(per_dev * c + per_dev - DROWS, CH), :], w2s.at[pl.ds(c * CH, CH), :], sem.at[1, c]))
        return out

    def run(wait):
        x = x_ref[...].reshape(TM, D)
        acc = None
        for c in range(n_ch):
            if wait:
                for cp in copies(c):
                    cp.wait()
            cs = pl.ds(c * CH, CH)
            a = gelu(dot(x, w1s[:, cs], 1, 0)).astype(BF16)
            part = dot(a, w2s[cs, :], 1, 0)
            acc = part if acc is None else acc + part
        o_ref[...] = (x.astype(F32) + acc).astype(BF16).reshape(o_ref.shape)

    @pl.when(i == 0)
    def _():
        for c in range(n_ch):
            for cp in copies(c):
                cp.start()
        run(True)

    @pl.when(i > 0)
    def _():
        run(False)


def fwd_call(stage, layer, x, w, y_prev):
    if layer == 0:
        x_spec = pl.BlockSpec((1, 1, TM, D), lambda i: (stage, 0, i, 0))
        out_shape = jax.ShapeDtypeStruct((TOK, D), BF16)
        o_spec = pl.BlockSpec((TM, D), lambda i: (i, 0))
    else:
        x_spec = pl.BlockSpec((TM, D), lambda i: (i, 0))
        out_shape = jax.ShapeDtypeStruct((2, 1, TOK, D), BF16)
        o_spec = pl.BlockSpec((1, 1, TM, D), lambda i: (stage, 0, i, 0))
    split = len(w) - 1
    args = [x, *w]
    specs = [x_spec] + [ANY] * len(w)
    aliases = {}
    if y_prev is not None:
        args.append(y_prev)
        specs.append(ANY)
        aliases = {2 + split: 0}
    return pl.pallas_call(
        functools.partial(fwd_kernel, len(aliases), split),
        out_shape=out_shape,
        grid_spec=pltpu.PrefetchScalarGridSpec(
            num_scalar_prefetch=0, grid=(NB,), in_specs=specs, out_specs=o_spec,
            scratch_shapes=[pltpu.VMEM((D, FF), BF16), pltpu.VMEM((FF, D), BF16), pltpu.SemaphoreType.DMA((2, FF // DROWS))]),
        input_output_aliases=aliases,
        compiler_params=pltpu.CompilerParams(dimension_semantics=("arbitrary",), vmem_limit_bytes=60 * 2 ** 20),
        cost_estimate=pl.CostEstimate(flops=4 * TOK * D * FF, bytes_accessed=26 * 2 ** 20, transcendentals=TOK * FF),
    )(*args)


SEQ = ("bwd_010a", "bwd_010b", "bwd_011", "bwd_110", "adam_01", "dx_01", "bwd_111", "bwd_000", "dx_11", "adam_11", "bwd_001", "bwd_100", "adam_00", "bwd_101", "adam_10", "fwd_00", "fwd_01", "fwd_10", "fwd_11")


def solution(mesh):
    tok_spec = P(None, 'fsdp')
    layer_spec = P(None, None, 'fsdp')
    n_dev = mesh.shape['fsdp']

    def swap(a, r):
        return lax.ppermute(a, 'fsdp', [(d, d ^ r) for d in range(n_dev)])

    def gather(a):
        return lax.all_gather(a, 'fsdp', axis=0, tiled=True)

    def device_step(x_saved, grad_out, x_next, w_up, w_down, acc_up, acc_down, master_up, master_down, moment1_up, moment1_down, moment2_up, moment2_down):
        me = lax.axis_index('fsdp').astype(jnp.int32)
        info = me.reshape(1)

        g_par = swap(grad_out, 1)
        x_par = swap(x_saved, 1)
        base_own = (x_saved, x_saved, grad_out, grad_out, w_up, w_down)
        base = (x_saved, x_par, grad_out, g_par, w_up, w_down)

        down5 = lambda a: a.reshape(2, 2, HALVES, BW, D)
        states = (acc_up, master_up, moment1_up, moment2_up, down5(acc_down), down5(master_down), down5(moment1_down), down5(moment2_down))

        recv = {}
        dx = {}
        dh = {}
        outs6 = ()
        full = {}
        hid = {}
        y = None

        for name in SEQ:
            s, l = int(name.split("_")[1][0]), int(name.split("_")[1][1])
            if name.startswith("adam"):
                split = (s, l) == (1, 1)
                res = adam_call(s, l, info, recv[s, l], states, outs6, split)
                outs6 = tuple(res[:6])
                if split:
                    late = res[7]
                    full[s, l] = [gather(res[6])]
                else:
                    full[s, l] = [gather(res[6])]
                if (s, l) == (1, 0):
                    full[1, 1].append(gather(lax.optimization_barrier((late, res[6]))[0]))
                continue
            if name.startswith("fwd"):
                if l == 0:
                    hid[s] = fwd_call(s, 0, x_next, full[s, 0], None)
                else:
                    y = fwd_call(s, 1, hid[s], full[s, 1], y)
                continue
            if name.startswith("dx"):
                own, par = dx_call(s, l, info, dh[s, 0], dh[s, 1], w_up)
                dx[s] = ((own, swap(par, 1)), (par, swap(own, 1)))
                continue
            half = int(name[6])
            if name == "bwd_010a":
                sum1, sum2, dh_own = bwd_call(s, l, half, 1, "own", info, base_own)
                continue
            if name == "bwd_010b":
                outs = bwd_call(s, l, half, 1, "par", info, base, sums=(sum1, sum2))
                dh[s, half] = (dh_own, outs[8])
            elif l == 0:
                outs = bwd_call(s, l, half, 3, "all", info, base, *dx[s])
            else:
                outs = bwd_call(s, l, half, 1, "all", info, base)
                dh[s, half] = tuple(outs[8:])
            msgs = [outs[0], outs[4], outs[1], outs[5], outs[2], outs[6], outs[3], outs[7]]
            recv.setdefault((s, l), []).append([msgs[0]] + [swap(msgs[r], r) for r in range(1, 8)])

        up4 = lambda a: a.reshape(2, 2, DROWS, D)
        return (outs6[0], up4(outs6[3]), outs6[1], up4(outs6[4]), outs6[2], up4(outs6[5]), y)

    return jax.shard_map(device_step, mesh=mesh, in_specs=(layer_spec, tok_spec, tok_spec, P(), P()) + (layer_spec,) * 8, out_specs=(layer_spec,) * 6 + (tok_spec,), check_vma=False)
```

```python
import functools
import math

import jax
import jax.numpy as jnp
from jax import lax
from jax.experimental import pallas as pl
from jax.experimental.pallas import tpu as pltpu
from jax.sharding import PartitionSpec as P


LEARN_RATE = 0.005
BETA_ONE = 0.9
BETA_TWO = 0.95
ADAM_EPS = 1e-8
WEIGHT_DECAY = 0.1
MICROBATCHES = 2
ADAM_STEP = 2
CORR_ONE = 1.0 - BETA_ONE ** ADAM_STEP
CORR_TWO = 1.0 - BETA_TWO ** ADAM_STEP
GELU_C = math.sqrt(2.0 / math.pi)
GELU_K = 0.044715

D = 1024
FF = 4096
TOK = 2048
TM = 512
NB = TOK // TM
HALVES = 2
FC = FF // 2 // HALVES
BW = FC // 4
ROWS = D // 8
DROWS = FF // 8

F32 = jnp.float32
BF16 = jnp.bfloat16

ANY = pl.BlockSpec(memory_space=pl.ANY)


def dot(a, b, ca, cb):
    return lax.dot_general(a, b, (((ca,), (cb,)), ((), ())), preferred_element_type=F32)


def gelu_pair(h):
    hh = h * h
    t = jnp.tanh(h * (GELU_C + (GELU_C * GELU_K) * hh))
    cdf = 0.5 * t + 0.5
    grad = cdf + h * ((0.5 - 0.5 * (t * t)) * (GELU_C + (3.0 * GELU_C * GELU_K) * hh))
    return h * cdf, grad


def gelu(h):
    t = jnp.tanh(h * (GELU_C + (GELU_C * GELU_K) * (h * h)))
    return h * (0.5 * t + 0.5)


def bwd_kernel(stage, layer, half, mode, part, info, *refs):
    it = iter(refs)
    take = lambda k: [next(it) for _ in range(k)]
    xo, xp, do, dp, w_up, w_down = take(6)
    n_extra = {1: 0, 3: 2}[mode]
    extra_own, extra_par = take(n_extra), take(n_extra)
    sums_in = take(2) if part == "par" else None
    if part == "own":
        sums_out = take(2)
    else:
        outs_even, outs_odd = take(4), take(4)
    if mode != 3:
        dho = next(it) if part != "par" else None
        dhp = next(it) if part != "own" else None
    xb, db, w1s, w2s, acc1, acc2, act, dhs, insem, wsem, ssem = take(11)
    eb, esem = take(2) if n_extra else (None, None)
    outsem = next(it) if mode != 3 else None
    i = pl.program_id(0)
    n = 2 * NB if part == "all" else NB
    base = NB if part == "par" else 0
    slot = lax.rem(i, 2)
    me = info[0]
    core = lax.rem(me, 2)
    chip = lax.div(me, 2)

    def in_copies(own, j, slot):
        rows = pl.ds(pl.multiple_of(j * TM, TM), TM)
        xs, ds, es = (xo, do, extra_own) if own else (xp, dp, extra_par)
        out = [pltpu.make_async_copy(xs.at[stage, layer, 0, rows], xb.at[slot], insem.at[0, slot]),
               pltpu.make_async_copy(ds.at[stage, 0, rows], db.at[slot], insem.at[1, slot])]
        for k, e in enumerate(es):
            out.append(pltpu.make_async_copy(e.at[rows], eb.at[k, slot], esem.at[k, slot]))
        return out

    def fetch(j, slot):
        @pl.when(j < NB)
        def _():
            for c in in_copies(True, j, slot):
                c.start()

        @pl.when(j >= NB)
        def _():
            for c in in_copies(False, j - NB, slot):
                c.start()

    def w_copies():
        out = []
        for j in range(4):
            f0 = pl.multiple_of(j * 1024 + core * 512 + half * BW, BW)
            out.append(pltpu.make_async_copy(w_up.at[stage, layer, :, pl.ds(f0, BW)], w1s.at[:, pl.ds(j * BW, BW)], wsem.at[0, j]))
            out.append(pltpu.make_async_copy(w_down.at[stage, layer, pl.ds(f0, BW), :], w2s.at[pl.ds(j * BW, BW), :], wsem.at[1, j]))
        return out

    @pl.when(i == 0)
    def _():
        fetch(base, 0)
        for c in w_copies():
            c.start()
        if part == "par":
            loads = [pltpu.make_async_copy(a, b, ssem.at[k]) for k, (a, b) in enumerate(zip(sums_in, (acc1, acc2)))]
            for c in loads:
                c.start()
            for c in loads:
                c.wait()
        else:
            acc1[...] = jnp.zeros_like(acc1)
            acc2[...] = jnp.zeros_like(acc2)
        for c in w_copies():
            c.wait()

    @pl.when(i + 1 < n)
    def _():
        fetch(base + i + 1, 1 - slot)

    for c in in_copies(True, 0, slot):
        c.wait()

    def dh_copy(own, j, slot):
        rows = pl.ds(pl.multiple_of(j * TM, TM), TM)
        return pltpu.make_async_copy(dhs.at[slot], (dho if own else dhp).at[rows], outsem.at[slot])

    if mode != 3:
        @pl.when(i >= 2)
        def _():
            dh_copy(part != "par", 0, slot).wait()

    CH = 256
    n_ch = FC // CH
    x = xb[slot]
    dy = db[slot]
    if mode == 3:
        dy = (dy.astype(F32) + (eb[0, slot] + eb[1, slot])).astype(BF16)

    def front(c):
        cs = slice(c * CH, (c + 1) * CH)
        h = dot(x, w1s[:, cs], 1, 0)
        da = dot(dy, w2s[cs, :], 1, 1)
        g, grad = gelu_pair(h)
        act[:, cs] = g.astype(BF16)
        dhs[slot, :, cs] = (da * grad).astype(BF16)

    def back(c):
        cs = slice(c * CH, (c + 1) * CH)
        acc1[:, cs] += dot(x, dhs[slot, :, cs], 0, 0)
        acc2[cs, :] += dot(act[:, cs], dy, 0, 0)

    for c in range(n_ch):
        front(c)
    for c in range(n_ch):
        back(c)
    if mode != 3:
        if part != "par":
            @pl.when(i < NB)
            def _():
                dh_copy(True, i, slot).start()

        if part != "own":
            @pl.when(i + base >= NB)
            def _():
                dh_copy(False, i + base - NB, slot).start()

    @pl.when(i == n - 1)
    def _():
        if part == "own":
            saves = [pltpu.make_async_copy(a, b, ssem.at[k]) for k, (a, b) in enumerate(zip((acc1, acc2), sums_out))]
            for c in saves:
                c.start()
            for c in saves:
                c.wait()
        else:
            for q in range(4):
                dev = jnp.bitwise_xor(me, 2 * q)
                oc = jnp.bitwise_xor(chip, q)
                outs_even[q][0:ROWS, :] = acc1[pl.ds(pl.multiple_of(dev * ROWS, ROWS), ROWS), :].astype(BF16)
                outs_even[q][ROWS:ROWS + BW, :] = acc2[pl.ds(pl.multiple_of(oc * BW, BW), BW), :].astype(BF16)
                dev = jnp.bitwise_xor(me, 2 * q + 1)
                outs_odd[q][...] = acc1[pl.ds(pl.multiple_of(dev * ROWS, ROWS), ROWS), :].astype(BF16)
        if mode != 3:
            dh_copy(part != "par", 0, 0).wait()
            dh_copy(part != "par", 0, 1).wait()


def bwd_call(stage, layer, half, mode, part, info, base_args, extra_own=(), extra_par=(), sums=()):
    sum_shapes = [jax.ShapeDtypeStruct((D, FC), F32), jax.ShapeDtypeStruct((FC, D), F32)]
    if part == "own":
        out_shape, out_specs = list(sum_shapes), [ANY] * 2
    else:
        out_shape = [jax.ShapeDtypeStruct((ROWS + BW, FC), BF16)] * 4 + [jax.ShapeDtypeStruct((ROWS, FC), BF16)] * 4
        out_specs = [pl.BlockSpec((ROWS + BW, FC), lambda i, s: (0, 0))] * 4 + [pl.BlockSpec((ROWS, FC), lambda i, s: (0, 0))] * 4
    scratch = [
        pltpu.VMEM((2, TM, D), BF16), pltpu.VMEM((2, TM, D), BF16),
        pltpu.VMEM((D, FC), BF16), pltpu.VMEM((FC, D), BF16),
        pltpu.VMEM((D, FC), F32), pltpu.VMEM((FC, D), F32),
        pltpu.VMEM((TM, FC), BF16), pltpu.VMEM((2, TM, FC), BF16),
        pltpu.SemaphoreType.DMA((2, 2)), pltpu.SemaphoreType.DMA((2, 4)), pltpu.SemaphoreType.DMA((2,)),
    ]
    args = list(base_args) + list(extra_own) + list(extra_par) + list(sums)
    n_extra = len(extra_own)
    if n_extra:
        scratch += [pltpu.VMEM((n_extra, 2, TM, D), F32), pltpu.SemaphoreType.DMA((n_extra, 2))]
    n_tok = 2 * TOK if part == "all" else TOK
    if mode != 3:
        k = 2 if part == "all" else 1
        out_shape += [jax.ShapeDtypeStruct((TOK, FC), BF16)] * k
        out_specs += [ANY] * k
        scratch += [pltpu.SemaphoreType.DMA((2,))]
    return pl.pallas_call(
        functools.partial(bwd_kernel, stage, layer, half, mode, part),
        out_shape=out_shape,
        grid_spec=pltpu.PrefetchScalarGridSpec(
            num_scalar_prefetch=1, grid=(n_tok // TM,), in_specs=[ANY] * len(args), out_specs=out_specs, scratch_shapes=scratch),
        compiler_params=pltpu.CompilerParams(dimension_semantics=("arbitrary",), vmem_limit_bytes=60 * 2 ** 20),
        cost_estimate=pl.CostEstimate(flops=8 * n_tok * D * FC, bytes_accessed=n_tok * 10 * 2 ** 10, transcendentals=n_tok * FC),
    )(info, *args)


def dx_kernel(stage, layer, info, h0o, h0p, h1o, h1p, w_up, dxo, dxp, dhb, w1s, dxb, insem, wsem, outsem):
    i = pl.program_id(0)
    n = 2 * NB
    slot = lax.rem(i, 2)
    core = lax.rem(info[0], 2)

    def in_copies(own, j, slot):
        rows = pl.ds(pl.multiple_of(j * TM, TM), TM)
        pair = (h0o, h1o) if own else (h0p, h1p)
        return [pltpu.make_async_copy(a.at[rows], dhb.at[slot, :, pl.ds(k * FC, FC)], insem.at[k, slot]) for k, a in enumerate(pair)]

    def fetch(j, slot):
        @pl.when(j < NB)
        def _():
            for c in in_copies(False, j, slot):
                c.start()

        @pl.when(j >= NB)
        def _():
            for c in in_copies(True, j - NB, slot):
                c.start()

    def w_copies():
        out = []
        for half in range(HALVES):
            for j in range(4):
                f0 = pl.multiple_of(j * 1024 + core * 512 + half * BW, BW)
                out.append(pltpu.make_async_copy(w_up.at[stage, layer, :, pl.ds(f0, BW)], w1s.at[:, pl.ds(half * FC + j * BW, BW)], wsem.at[half, j]))
        return out

    def out_copy(own, j, slot):
        rows = pl.ds(pl.multiple_of(j * TM, TM), TM)
        return pltpu.make_async_copy(dxb.at[slot], (dxo if own else dxp).at[rows], outsem.at[slot])

    @pl.when(i == 0)
    def _():
        fetch(0, 0)
        for c in w_copies():
            c.start()
        for c in w_copies():
            c.wait()

    @pl.when(i + 1 < n)
    def _():
        fetch(i + 1, 1 - slot)

    for c in in_copies(True, 0, slot):
        c.wait()

    @pl.when(i >= 2)
    def _():
        out_copy(True, 0, slot).wait()

    dxb[slot] = dot(dhb[slot], w1s[...], 1, 1)

    @pl.when(i < NB)
    def _():
        out_copy(False, i, slot).start()

    @pl.when(i >= NB)
    def _():
        out_copy(True, i - NB, slot).start()

    @pl.when(i == n - 1)
    def _():
        out_copy(True, 0, 0).wait()
        out_copy(True, 0, 1).wait()


def dx_call(stage, layer, info, dh0, dh1, w_up):
    args = [dh0[0], dh0[1], dh1[0], dh1[1], w_up]
    return pl.pallas_call(
        functools.partial(dx_kernel, stage, layer),
        out_shape=[jax.ShapeDtypeStruct((TOK, D), F32)] * 2,
        grid_spec=pltpu.PrefetchScalarGridSpec(
            num_scalar_prefetch=1, grid=(2 * NB,), in_specs=[ANY] * 5, out_specs=[ANY] * 2,
            scratch_shapes=[pltpu.VMEM((2, TM, HALVES * FC), BF16), pltpu.VMEM((D, HALVES * FC), BF16), pltpu.VMEM((2, TM, D), F32),
                            pltpu.SemaphoreType.DMA((2, 2)), pltpu.SemaphoreType.DMA((2, 4)), pltpu.SemaphoreType.DMA((2,))]),
        compiler_params=pltpu.CompilerParams(dimension_semantics=("arbitrary",), vmem_limit_bytes=60 * 2 ** 20),
        cost_estimate=pl.CostEstimate(flops=4 * TOK * D * HALVES * FC, bytes_accessed=38 * 2 ** 20, transcendentals=0),
    )(info, *args)


def adam(grad_new, acc, master, m1, m2):
    g = (acc + grad_new) / MICROBATCHES
    m1 = BETA_ONE * m1 + (1.0 - BETA_ONE) * g
    m2 = BETA_TWO * m2 + (1.0 - BETA_TWO) * g * g
    step_dir = (m1 * (1.0 / CORR_ONE)) / (jnp.sqrt(m2 * (1.0 / CORR_TWO)) + ADAM_EPS)
    master = master - LEARN_RATE * (step_dir + WEIGHT_DECAY * master)
    return master, m1, m2


def adam_kernel(n_alias, split, info, *refs):
    up = refs[:16]
    down = refs[16:24]
    au, mu, m1u, m2u, ad, md, m1d, m2d = refs[24:32]
    omu, om1u, om2u, omd, om1d, om2d = refs[32 + n_alias:38 + n_alias]
    w_up_out, w_down_out = refs[38 + n_alias], refs[-1]
    down0 = 0 if split else DROWS
    core = lax.rem(info[0], 2)
    j = pl.program_id(0)
    up_rows = pl.ds(pl.multiple_of(j * ROWS, ROWS), ROWS)
    for half in range(HALVES):
        for g in range(2):
            total = None
            for q in range(4):
                v = up[half * 8 + 2 * q + g][...].astype(F32)
                total = v if total is None else total + v
            col = jnp.bitwise_xor(core, g) * 512 + half * BW
            cs = pl.ds(pl.multiple_of(col, BW), BW)
            new = adam(total, au[0, 0, :, cs], mu[0, 0, :, cs], m1u[0, 0, :, cs], m2u[0, 0, :, cs])
            omu[0, 0, :, cs] = new[0]
            om1u[0, 0, :, cs] = new[1]
            om2u[0, 0, :, cs] = new[2]
            w_up_out[up_rows, cs] = new[0].astype(BF16)
        total = None
        for q in range(4):
            v = down[half * 4 + q][...].astype(F32)
            total = v if total is None else total + v
        new = adam(total, ad[0, 0, half], md[0, 0, half], m1d[0, 0, half], m2d[0, 0, half])
        omd[0, 0, half] = new[0]
        om1d[0, 0, half] = new[1]
        om2d[0, 0, half] = new[2]
        w_down_out[pl.ds(pl.multiple_of(down0 + half * BW + j * (BW // 4), BW // 4), BW // 4), :] = new[0].astype(BF16)


def adam_call(stage, layer, info, recv, states, prev, split):
    nj = 4
    dr = BW // nj
    up_spec = pl.BlockSpec((ROWS, BW), lambda j, s: (0, j))
    down_spec = pl.BlockSpec((dr, D), lambda j, s: (ROWS // dr + j, 0))
    st_up = pl.BlockSpec((1, 1, ROWS, FF // nj), lambda j, s: (stage, layer, 0, j))
    st_down = pl.BlockSpec((1, 1, HALVES, dr, D), lambda j, s: (stage, layer, 0, j, 0))
    args, specs = [], []
    for half in range(HALVES):
        for r in range(8):
            args.append(recv[half][r])
            specs.append(up_spec)
    for half in range(HALVES):
        for q in range(4):
            args.append(recv[half][2 * q])
            specs.append(down_spec)
    args += list(states)
    specs += [st_up] * 4 + [st_down] * 4
    n_alias = len(prev)
    args += list(prev)
    specs += [ANY] * n_alias
    up_shape = jax.ShapeDtypeStruct(states[0].shape, F32)
    down_shape = jax.ShapeDtypeStruct(states[4].shape, F32)
    n_in = 1 + len(args) - n_alias
    w_shapes = [jax.ShapeDtypeStruct((DROWS, D), BF16)] * 2 if split else [jax.ShapeDtypeStruct((2 * DROWS, D), BF16)]
    return pl.pallas_call(
        functools.partial(adam_kernel, n_alias, split),
        out_shape=[up_shape] * 3 + [down_shape] * 3 + w_shapes,
        grid_spec=pltpu.PrefetchScalarGridSpec(
            num_scalar_prefetch=1, grid=(nj,), in_specs=specs,
            out_specs=[st_up] * 3 + [st_down] * 3 + [pl.BlockSpec(w.shape, lambda j, s: (0, 0)) for w in w_shapes]),
        input_output_aliases={n_in + k: k for k in range(n_alias)},
        compiler_params=pltpu.CompilerParams(dimension_semantics=("arbitrary",), vmem_limit_bytes=60 * 2 ** 20),
        cost_estimate=pl.CostEstimate(flops=20 * 2 ** 20 * 40, bytes_accessed=40 * 2 ** 20, transcendentals=2 ** 20),
    )(info, *args)


def fwd_kernel(has_alias, *refs):
    x_ref, w = refs[:2]
    o_ref, w1s, w2s, sem = refs[2 + has_alias:]
    i = pl.program_id(0)
    CH = DROWS
    n_ch = FF // CH

    def copies(c):
        out = up_copies(w, 2 * DROWS, c, w1s, sem.at[0, c])
        out.append(pltpu.make_async_copy(w.at[pl.ds(2 * DROWS * c + DROWS, CH), :], w2s.at[pl.ds(c * CH, CH), :], sem.at[1, c]))
        return out

    def run(wait):
        x = x_ref[...].reshape(TM, D)
        acc = None
        for c in range(n_ch):
            if wait:
                for cp in copies(c):
                    cp.wait()
            cs = pl.ds(c * CH, CH)
            a = gelu(dot(x, w1s[:, cs], 1, 0)).astype(BF16)
            part = dot(a, w2s[cs, :], 1, 0)
            acc = part if acc is None else acc + part
        o_ref[...] = (x.astype(F32) + acc).astype(BF16).reshape(o_ref.shape)

    @pl.when(i == 0)
    def _():
        for c in range(n_ch):
            for cp in copies(c):
                cp.start()
        run(True)

    @pl.when(i > 0)
    def _():
        run(False)


def up_copies(w, per_dev, c, w1s, sem):
    out = []
    for d in range(8):
        src = w.at[pl.ds(per_dev * d + (c // 2) * ROWS, ROWS), pl.ds((c % 2) * DROWS, DROWS)]
        out.append(pltpu.make_async_copy(src, w1s.at[pl.ds(d * ROWS, ROWS), pl.ds(c * DROWS, DROWS)], sem))
    return out


def first_kernel(x_ref, wu, a_ref, w1s, sem):
    i = pl.program_id(0)
    CH = DROWS
    n_ch = FF // CH

    def run(wait):
        x = x_ref[...].reshape(TM, D)
        for c in range(n_ch):
            if wait:
                for cp in up_copies(wu, DROWS, c, w1s, sem.at[c]):
                    cp.wait()
            cs = pl.ds(c * CH, CH)
            a_ref[:, cs] = gelu(dot(x, w1s[:, cs], 1, 0)).astype(BF16)

    @pl.when(i == 0)
    def _():
        for c in range(n_ch):
            for cp in up_copies(wu, DROWS, c, w1s, sem.at[c]):
                cp.start()
        run(True)

    @pl.when(i > 0)
    def _():
        run(False)


def second_kernel(has_alias, *refs):
    x_ref, a_ref, wd = refs[:3]
    o_ref, w2s, sem = refs[3 + has_alias:]
    i = pl.program_id(0)
    KH = FF // 4

    def copy(c):
        return pltpu.make_async_copy(wd.at[pl.ds(c * KH, KH), :], w2s.at[pl.ds(c * KH, KH), :], sem.at[c])

    def store(acc):
        x = x_ref[...].reshape(TM, D)
        o_ref[...] = (x.astype(F32) + acc).astype(BF16).reshape(o_ref.shape)

    @pl.when(i == 0)
    def _():
        for c in range(4):
            copy(c).start()
        acc = None
        for c in range(4):
            copy(c).wait()
            part = dot(a_ref[:, pl.ds(c * KH, KH)], w2s[pl.ds(c * KH, KH), :], 1, 0)
            acc = part if acc is None else acc + part
        store(acc)

    @pl.when(i > 0)
    def _():
        store(dot(a_ref[...], w2s[...], 1, 0))


def x_spec_of(stage, layer):
    if layer == 0:
        return pl.BlockSpec((1, 1, TM, D), lambda i: (stage, 0, i, 0))
    return pl.BlockSpec((TM, D), lambda i: (i, 0))


def out_of(stage, layer):
    if layer == 0:
        return jax.ShapeDtypeStruct((TOK, D), BF16), pl.BlockSpec((TM, D), lambda i: (i, 0))
    return jax.ShapeDtypeStruct((2, 1, TOK, D), BF16), pl.BlockSpec((1, 1, TM, D), lambda i: (stage, 0, i, 0))


def token_call(body, args, specs, out, y_prev, scratch, flops):
    out_shape, o_spec = out
    aliases = {}
    if y_prev is not None:
        aliases = {len(args): 0}
        args, specs = args + [y_prev], specs + [ANY]
    if body is not first_kernel:
        body = functools.partial(body, len(aliases))
    return pl.pallas_call(
        body,
        out_shape=out_shape,
        grid_spec=pltpu.PrefetchScalarGridSpec(num_scalar_prefetch=0, grid=(NB,), in_specs=specs, out_specs=o_spec, scratch_shapes=scratch),
        input_output_aliases=aliases,
        compiler_params=pltpu.CompilerParams(dimension_semantics=("arbitrary",), vmem_limit_bytes=60 * 2 ** 20),
        cost_estimate=pl.CostEstimate(flops=flops, bytes_accessed=26 * 2 ** 20, transcendentals=TOK * FF),
    )(*args)


def fwd_call(stage, layer, x, w, y_prev):
    scratch = [pltpu.VMEM((D, FF), BF16), pltpu.VMEM((FF, D), BF16), pltpu.SemaphoreType.DMA((2, FF // DROWS))]
    return token_call(fwd_kernel, [x, w], [x_spec_of(stage, layer), ANY], out_of(stage, layer), y_prev, scratch, 4 * TOK * D * FF)


def first_call(stage, layer, x, wu):
    scratch = [pltpu.VMEM((D, FF), BF16), pltpu.SemaphoreType.DMA((FF // DROWS,))]
    out = jax.ShapeDtypeStruct((TOK, FF), BF16), pl.BlockSpec((TM, FF), lambda i: (i, 0))
    return token_call(first_kernel, [x, wu], [x_spec_of(stage, layer), ANY], out, None, scratch, 2 * TOK * D * FF)


def second_call(stage, layer, x, act, wd, y_prev):
    scratch = [pltpu.VMEM((FF, D), BF16), pltpu.SemaphoreType.DMA((4,))]
    specs = [x_spec_of(stage, layer), pl.BlockSpec((TM, FF), lambda i: (i, 0)), ANY]
    return token_call(second_kernel, [x, act, wd], specs, out_of(stage, layer), y_prev, scratch, 2 * TOK * D * FF)


SEQ = ("bwd_010a", "bwd_010b", "bwd_011", "bwd_110", "adam_01", "dx_01", "bwd_111", "bwd_000", "bwd_001", "dx_11", "adam_11", "adam_00", "bwd_100", "bwd_101", "fwd_00", "adam_10", "fwd_01", "fwd_10a", "fwd_10b", "fwd_11a", "fwd_11b")


def solution(mesh):
    tok_spec = P(None, 'fsdp')
    layer_spec = P(None, None, 'fsdp')
    n_dev = mesh.shape['fsdp']

    def swap(a, r):
        return lax.ppermute(a, 'fsdp', [(d, d ^ r) for d in range(n_dev)])

    def gather(a):
        return lax.all_gather(a, 'fsdp', axis=0, tiled=True)

    def device_step(x_saved, grad_out, x_next, w_up, w_down, acc_up, acc_down, master_up, master_down, moment1_up, moment1_down, moment2_up, moment2_down):
        me = lax.axis_index('fsdp').astype(jnp.int32)
        info = me.reshape(1)

        g_par = swap(grad_out, 1)
        x_par = swap(x_saved, 1)
        base_own = (x_saved, x_saved, grad_out, grad_out, w_up, w_down)
        base = (x_saved, x_par, grad_out, g_par, w_up, w_down)

        down5 = lambda a: a.reshape(2, 2, HALVES, BW, D)
        states = (acc_up, master_up, moment1_up, moment2_up, down5(acc_down), down5(master_down), down5(moment1_down), down5(moment2_down))

        recv = {}
        dx = {}
        dh = {}
        outs6 = ()
        full = {}
        hid = {}
        y = None

        for name in SEQ:
            s, l = int(name.split("_")[1][0]), int(name.split("_")[1][1])
            if name.startswith("adam"):
                res = adam_call(s, l, info, recv[s, l], states, outs6, s == 1)
                outs6 = tuple(res[:6])
                w_new = res[6:]
                if (s, l) == (1, 1):
                    late = w_new
                elif (s, l) == (1, 0):
                    full[s, l] = [gather(w_new[0]), gather(w_new[1])]
                    full[1, 1].append(gather(lax.optimization_barrier((late[1], w_new[0]))[0]))
                else:
                    full[s, l] = gather(w_new[0])
                if (s, l) == (0, 0):
                    full[1, 1] = [gather(lax.optimization_barrier((late[0], w_new[0]))[0])]
                continue
            if name.startswith("fwd"):
                x_in = x_next if l == 0 else hid[s]
                y_prev = y if l == 1 else None
                if name.endswith("a"):
                    act = first_call(s, l, x_in, full[s, l][0])
                    continue
                if name.endswith("b"):
                    out = second_call(s, l, x_in, act, full[s, l][1], y_prev)
                else:
                    out = fwd_call(s, l, x_in, full[s, l], y_prev)
                if l == 0:
                    hid[s] = out
                else:
                    y = out
                continue
            if name.startswith("dx"):
                own, par = dx_call(s, l, info, dh[s, 0], dh[s, 1], w_up)
                dx[s] = ((own, swap(par, 1)), (par, swap(own, 1)))
                continue
            half = int(name[6])
            if name == "bwd_010a":
                sum1, sum2, dh_own = bwd_call(s, l, half, 1, "own", info, base_own)
                continue
            if name == "bwd_010b":
                outs = bwd_call(s, l, half, 1, "par", info, base, sums=(sum1, sum2))
                dh[s, half] = (dh_own, outs[8])
            elif l == 0:
                outs = bwd_call(s, l, half, 3, "all", info, base, *dx[s])
            else:
                outs = bwd_call(s, l, half, 1, "all", info, base)
                dh[s, half] = tuple(outs[8:])
            msgs = [outs[0], outs[4], outs[1], outs[5], outs[2], outs[6], outs[3], outs[7]]
            recv.setdefault((s, l), []).append([msgs[0]] + [swap(msgs[r], r) for r in range(1, 8)])

        up4 = lambda a: a.reshape(2, 2, DROWS, D)
        return (outs6[0], up4(outs6[3]), outs6[1], up4(outs6[4]), outs6[2], up4(outs6[5]), y)

    return jax.shard_map(device_step, mesh=mesh, in_specs=(layer_spec, tok_spec, tok_spec, P(), P()) + (layer_spec,) * 8, out_specs=(layer_spec,) * 6 + (tok_spec,), check_vma=False)
```

```python
import functools
import math

import jax
import jax.numpy as jnp
from jax import lax
from jax.experimental import pallas as pl
from jax.experimental.pallas import tpu as pltpu
from jax.sharding import PartitionSpec as P


LEARN_RATE = 0.005
BETA_ONE = 0.9
BETA_TWO = 0.95
ADAM_EPS = 1e-8
WEIGHT_DECAY = 0.1
MICROBATCHES = 2
ADAM_STEP = 2
CORR_ONE = 1.0 - BETA_ONE ** ADAM_STEP
CORR_TWO = 1.0 - BETA_TWO ** ADAM_STEP
GELU_C = math.sqrt(2.0 / math.pi)
GELU_K = 0.044715

D = 1024
FF = 4096
TOK = 2048
TM = 512
NB = TOK // TM
HALVES = 2
FC = FF // 2 // HALVES
BW = FC // 4
ROWS = D // 8
DROWS = FF // 8

F32 = jnp.float32
BF16 = jnp.bfloat16

ANY = pl.BlockSpec(memory_space=pl.ANY)


def dot(a, b, ca, cb):
    return lax.dot_general(a, b, (((ca,), (cb,)), ((), ())), preferred_element_type=F32)


def gelu_pair(h):
    hh = h * h
    t = jnp.tanh(h * (GELU_C + (GELU_C * GELU_K) * hh))
    cdf = 0.5 * t + 0.5
    grad = cdf + h * ((0.5 - 0.5 * (t * t)) * (GELU_C + (3.0 * GELU_C * GELU_K) * hh))
    return h * cdf, grad


def gelu(h):
    t = jnp.tanh(h * (GELU_C + (GELU_C * GELU_K) * (h * h)))
    return h * (0.5 * t + 0.5)


def flip(v, mask):
    total = 0
    for b in range(3):
        bit = lax.rem(lax.div(v, 2 ** b), 2)
        total = total + 2 ** b * (1 - bit if (mask >> b) & 1 else bit)
    return total


def bwd_kernel(stage, layer, half, mode, part, *refs):
    it = iter(refs)
    take = lambda k: [next(it) for _ in range(k)]
    info = next(it) if part == "all" else None
    if part == "all":
        xo, xp, do, dp, w_up, w_down = take(6)
    else:
        xo, do, w_up, w_down = take(4)
    n_extra = {1: 0, 3: 2}[mode]
    extra_own, extra_par = take(n_extra), take(n_extra)
    outs_even, outs_odd = take(4), take(4)
    if mode != 3:
        dho, dhp = take(2)
    if part == "swap":
        xp, dp = take(2)
    xb, db, w1s, w2s, acc1, acc2, act, dhs, insem, wsem = take(10)
    eb, esem = take(2) if n_extra else (None, None)
    outsem = next(it) if mode != 3 else None
    if part == "swap":
        send_sem, recv_sem = take(2)
    i = pl.program_id(0)
    n = 2 * NB
    slot = lax.rem(i, 2)
    me = info[0] if part == "all" else lax.axis_index('fsdp')
    core = lax.rem(me, 2)
    chip = lax.div(me, 2)
    partner = flip(me, 1)

    def in_copies(own, j, slot):
        rows = pl.ds(pl.multiple_of(j * TM, TM), TM)
        xs, ds, es = (xo, do, extra_own) if own else (xp, dp, extra_par)
        xs = xs.at[rows] if len(xs.shape) == 2 else xs.at[stage, layer, 0, rows]
        ds = ds.at[rows] if len(ds.shape) == 2 else ds.at[stage, 0, rows]
        out = [pltpu.make_async_copy(xs, xb.at[slot], insem.at[0, slot]),
               pltpu.make_async_copy(ds, db.at[slot], insem.at[1, slot])]
        for k, e in enumerate(es):
            out.append(pltpu.make_async_copy(e.at[rows], eb.at[k, slot], esem.at[k, slot]))
        return out

    def fetch(j, slot):
        @pl.when(j < NB)
        def _():
            for c in in_copies(True, j, slot):
                c.start()

        @pl.when(j >= NB)
        def _():
            for c in in_copies(False, j - NB, slot):
                c.start()

    def w_copies():
        out = []
        for j in range(4):
            f0 = pl.multiple_of(j * 1024 + core * 512 + half * BW, BW)
            out.append(pltpu.make_async_copy(w_up.at[stage, layer, :, pl.ds(f0, BW)], w1s.at[:, pl.ds(j * BW, BW)], wsem.at[0, j]))
            out.append(pltpu.make_async_copy(w_down.at[stage, layer, pl.ds(f0, BW), :], w2s.at[pl.ds(j * BW, BW), :], wsem.at[1, j]))
        return out

    def swap_copies():
        pairs = ((xo.at[stage, layer, 0], xp), (do.at[stage, 0], dp))
        return [pltpu.make_async_remote_copy(src_ref=a, dst_ref=b, send_sem=send_sem.at[k], recv_sem=recv_sem.at[k], device_id=(partner,), device_id_type=pl.DeviceIdType.MESH)
                for k, (a, b) in enumerate(pairs)]

    @pl.when(i == 0)
    def _():
        fetch(0, 0)
        for c in w_copies():
            c.start()
        if part == "swap":
            barrier = pltpu.get_barrier_semaphore()
            pl.semaphore_signal(barrier, inc=1, device_id=(partner,), device_id_type=pl.DeviceIdType.MESH)
            pl.semaphore_wait(barrier, 1)
            for c in swap_copies():
                c.start()
        acc1[...] = jnp.zeros_like(acc1)
        acc2[...] = jnp.zeros_like(acc2)
        for c in w_copies():
            c.wait()

    if part == "swap":
        @pl.when(i == NB - 1)
        def _():
            for c in swap_copies():
                c.wait()

    @pl.when(i + 1 < n)
    def _():
        fetch(i + 1, 1 - slot)

    for c in in_copies(True, 0, slot):
        c.wait()

    def dh_copy(own, j, slot):
        rows = pl.ds(pl.multiple_of(j * TM, TM), TM)
        return pltpu.make_async_copy(dhs.at[slot], (dho if own else dhp).at[rows], outsem.at[slot])

    if mode != 3:
        @pl.when(i >= 2)
        def _():
            dh_copy(True, 0, slot).wait()

    CH = 256
    n_ch = FC // CH
    x = xb[slot]
    dy = db[slot]
    if mode == 3:
        dy = (dy.astype(F32) + (eb[0, slot] + eb[1, slot])).astype(BF16)

    def front(c):
        cs = slice(c * CH, (c + 1) * CH)
        h = dot(x, w1s[:, cs], 1, 0)
        da = dot(dy, w2s[cs, :], 1, 1)
        g, grad = gelu_pair(h)
        act[:, cs] = g.astype(BF16)
        dhs[slot, :, cs] = (da * grad).astype(BF16)

    def back(c):
        cs = slice(c * CH, (c + 1) * CH)
        acc1[:, cs] += dot(x, dhs[slot, :, cs], 0, 0)
        acc2[cs, :] += dot(act[:, cs], dy, 0, 0)

    for c in range(n_ch):
        front(c)
    for c in range(n_ch):
        back(c)
    if mode != 3:
        @pl.when(i < NB)
        def _():
            dh_copy(True, i, slot).start()

        @pl.when(i >= NB)
        def _():
            dh_copy(False, i - NB, slot).start()

    @pl.when(i == n - 1)
    def _():
        for q in range(4):
            dev = flip(me, 2 * q)
            oc = flip(chip, q)
            outs_even[q][0:ROWS, :] = acc1[pl.ds(pl.multiple_of(dev * ROWS, ROWS), ROWS), :].astype(BF16)
            outs_even[q][ROWS:ROWS + BW, :] = acc2[pl.ds(pl.multiple_of(oc * BW, BW), BW), :].astype(BF16)
            dev = flip(me, 2 * q + 1)
            outs_odd[q][...] = acc1[pl.ds(pl.multiple_of(dev * ROWS, ROWS), ROWS), :].astype(BF16)
        if mode != 3:
            dh_copy(True, 0, 0).wait()
            dh_copy(True, 0, 1).wait()


def bwd_call(stage, layer, half, mode, part, info, base_args, extra_own=(), extra_par=()):
    out_shape = [jax.ShapeDtypeStruct((ROWS + BW, FC), BF16)] * 4 + [jax.ShapeDtypeStruct((ROWS, FC), BF16)] * 4
    out_specs = [pl.BlockSpec((ROWS + BW, FC), lambda *_: (0, 0))] * 4 + [pl.BlockSpec((ROWS, FC), lambda *_: (0, 0))] * 4
    scratch = [
        pltpu.VMEM((2, TM, D), BF16), pltpu.VMEM((2, TM, D), BF16),
        pltpu.VMEM((D, FC), BF16), pltpu.VMEM((FC, D), BF16),
        pltpu.VMEM((D, FC), F32), pltpu.VMEM((FC, D), F32),
        pltpu.VMEM((TM, FC), BF16), pltpu.VMEM((2, TM, FC), BF16),
        pltpu.SemaphoreType.DMA((2, 2)), pltpu.SemaphoreType.DMA((2, 4)),
    ]
    args = list(base_args) + list(extra_own) + list(extra_par)
    n_extra = len(extra_own)
    if n_extra:
        scratch += [pltpu.VMEM((n_extra, 2, TM, D), F32), pltpu.SemaphoreType.DMA((n_extra, 2))]
    if mode != 3:
        out_shape += [jax.ShapeDtypeStruct((TOK, FC), BF16)] * 2
        out_specs += [ANY] * 2
        scratch += [pltpu.SemaphoreType.DMA((2,))]
    params = dict(dimension_semantics=("arbitrary",), vmem_limit_bytes=60 * 2 ** 20)
    if part == "swap":
        out_shape += [jax.ShapeDtypeStruct((TOK, D), BF16)] * 2
        out_specs += [ANY] * 2
        scratch += [pltpu.SemaphoreType.DMA((2,)), pltpu.SemaphoreType.DMA((2,))]
        params.update(collective_id=0, has_side_effects=True)
    call = pl.pallas_call(
        functools.partial(bwd_kernel, stage, layer, half, mode, part),
        out_shape=out_shape,
        grid_spec=pltpu.PrefetchScalarGridSpec(
            num_scalar_prefetch=int(part == "all"), grid=(2 * NB,), in_specs=[ANY] * len(args), out_specs=out_specs, scratch_shapes=scratch),
        compiler_params=pltpu.CompilerParams(**params),
        cost_estimate=pl.CostEstimate(flops=16 * TOK * D * FC, bytes_accessed=40 * 2 ** 20, transcendentals=2 * TOK * FC),
    )
    return call(*args) if part == "swap" else call(info, *args)


def dx_kernel(stage, layer, info, h0o, h0p, h1o, h1p, w_up, dxo, dxp, dhb, w1s, dxb, insem, wsem, outsem):
    i = pl.program_id(0)
    n = 2 * NB
    slot = lax.rem(i, 2)
    core = lax.rem(info[0], 2)

    def in_copies(own, j, slot):
        rows = pl.ds(pl.multiple_of(j * TM, TM), TM)
        pair = (h0o, h1o) if own else (h0p, h1p)
        return [pltpu.make_async_copy(a.at[rows], dhb.at[slot, :, pl.ds(k * FC, FC)], insem.at[k, slot]) for k, a in enumerate(pair)]

    def fetch(j, slot):
        @pl.when(j < NB)
        def _():
            for c in in_copies(False, j, slot):
                c.start()

        @pl.when(j >= NB)
        def _():
            for c in in_copies(True, j - NB, slot):
                c.start()

    def w_copies():
        out = []
        for half in range(HALVES):
            for j in range(4):
                f0 = pl.multiple_of(j * 1024 + core * 512 + half * BW, BW)
                out.append(pltpu.make_async_copy(w_up.at[stage, layer, :, pl.ds(f0, BW)], w1s.at[:, pl.ds(half * FC + j * BW, BW)], wsem.at[half, j]))
        return out

    def out_copy(own, j, slot):
        rows = pl.ds(pl.multiple_of(j * TM, TM), TM)
        return pltpu.make_async_copy(dxb.at[slot], (dxo if own else dxp).at[rows], outsem.at[slot])

    @pl.when(i == 0)
    def _():
        fetch(0, 0)
        for c in w_copies():
            c.start()
        for c in w_copies():
            c.wait()

    @pl.when(i + 1 < n)
    def _():
        fetch(i + 1, 1 - slot)

    for c in in_copies(True, 0, slot):
        c.wait()

    @pl.when(i >= 2)
    def _():
        out_copy(True, 0, slot).wait()

    dxb[slot] = dot(dhb[slot], w1s[...], 1, 1)

    @pl.when(i < NB)
    def _():
        out_copy(False, i, slot).start()

    @pl.when(i >= NB)
    def _():
        out_copy(True, i - NB, slot).start()

    @pl.when(i == n - 1)
    def _():
        out_copy(True, 0, 0).wait()
        out_copy(True, 0, 1).wait()


def dx_call(stage, layer, info, dh0, dh1, w_up):
    args = [dh0[0], dh0[1], dh1[0], dh1[1], w_up]
    return pl.pallas_call(
        functools.partial(dx_kernel, stage, layer),
        out_shape=[jax.ShapeDtypeStruct((TOK, D), F32)] * 2,
        grid_spec=pltpu.PrefetchScalarGridSpec(
            num_scalar_prefetch=1, grid=(2 * NB,), in_specs=[ANY] * 5, out_specs=[ANY] * 2,
            scratch_shapes=[pltpu.VMEM((2, TM, HALVES * FC), BF16), pltpu.VMEM((D, HALVES * FC), BF16), pltpu.VMEM((2, TM, D), F32),
                            pltpu.SemaphoreType.DMA((2, 2)), pltpu.SemaphoreType.DMA((2, 4)), pltpu.SemaphoreType.DMA((2,))]),
        compiler_params=pltpu.CompilerParams(dimension_semantics=("arbitrary",), vmem_limit_bytes=60 * 2 ** 20),
        cost_estimate=pl.CostEstimate(flops=4 * TOK * D * HALVES * FC, bytes_accessed=38 * 2 ** 20, transcendentals=0),
    )(info, *args)


def adam(grad_new, acc, master, m1, m2):
    g = (acc + grad_new) / MICROBATCHES
    m1 = BETA_ONE * m1 + (1.0 - BETA_ONE) * g
    m2 = BETA_TWO * m2 + (1.0 - BETA_TWO) * g * g
    step_dir = (m1 * (1.0 / CORR_ONE)) / (jnp.sqrt(m2 * (1.0 / CORR_TWO)) + ADAM_EPS)
    master = master - LEARN_RATE * (step_dir + WEIGHT_DECAY * master)
    return master, m1, m2


def adam_kernel(n_alias, split, info, *refs):
    up = refs[:16]
    down = refs[16:24]
    au, mu, m1u, m2u, ad, md, m1d, m2d = refs[24:32]
    omu, om1u, om2u, omd, om1d, om2d = refs[32 + n_alias:38 + n_alias]
    w_up_out, w_down_out = refs[38 + n_alias], refs[-1]
    down0 = 0 if split else DROWS
    core = lax.rem(info[0], 2)
    j = pl.program_id(0)
    up_rows = pl.ds(pl.multiple_of(j * ROWS, ROWS), ROWS)
    for half in range(HALVES):
        for g in range(2):
            total = None
            for q in range(4):
                v = up[half * 8 + 2 * q + g][...].astype(F32)
                total = v if total is None else total + v
            col = jnp.bitwise_xor(core, g) * 512 + half * BW
            cs = pl.ds(pl.multiple_of(col, BW), BW)
            new = adam(total, au[0, 0, :, cs], mu[0, 0, :, cs], m1u[0, 0, :, cs], m2u[0, 0, :, cs])
            omu[0, 0, :, cs] = new[0]
            om1u[0, 0, :, cs] = new[1]
            om2u[0, 0, :, cs] = new[2]
            w_up_out[up_rows, cs] = new[0].astype(BF16)
        total = None
        for q in range(4):
            v = down[half * 4 + q][...].astype(F32)
            total = v if total is None else total + v
        new = adam(total, ad[0, 0, half], md[0, 0, half], m1d[0, 0, half], m2d[0, 0, half])
        omd[0, 0, half] = new[0]
        om1d[0, 0, half] = new[1]
        om2d[0, 0, half] = new[2]
        w_down_out[pl.ds(pl.multiple_of(down0 + half * BW + j * (BW // 4), BW // 4), BW // 4), :] = new[0].astype(BF16)


def adam_call(stage, layer, info, recv, states, prev, split):
    nj = 4
    dr = BW // nj
    up_spec = pl.BlockSpec((ROWS, BW), lambda j, s: (0, j))
    down_spec = pl.BlockSpec((dr, D), lambda j, s: (ROWS // dr + j, 0))
    st_up = pl.BlockSpec((1, 1, ROWS, FF // nj), lambda j, s: (stage, layer, 0, j))
    st_down = pl.BlockSpec((1, 1, HALVES, dr, D), lambda j, s: (stage, layer, 0, j, 0))
    args, specs = [], []
    for half in range(HALVES):
        for r in range(8):
            args.append(recv[half][r])
            specs.append(up_spec)
    for half in range(HALVES):
        for q in range(4):
            args.append(recv[half][2 * q])
            specs.append(down_spec)
    args += list(states)
    specs += [st_up] * 4 + [st_down] * 4
    n_alias = len(prev)
    args += list(prev)
    specs += [ANY] * n_alias
    up_shape = jax.ShapeDtypeStruct(states[0].shape, F32)
    down_shape = jax.ShapeDtypeStruct(states[4].shape, F32)
    n_in = 1 + len(args) - n_alias
    w_shapes = [jax.ShapeDtypeStruct((DROWS, D), BF16)] * 2 if split else [jax.ShapeDtypeStruct((2 * DROWS, D), BF16)]
    return pl.pallas_call(
        functools.partial(adam_kernel, n_alias, split),
        out_shape=[up_shape] * 3 + [down_shape] * 3 + w_shapes,
        grid_spec=pltpu.PrefetchScalarGridSpec(
            num_scalar_prefetch=1, grid=(nj,), in_specs=specs,
            out_specs=[st_up] * 3 + [st_down] * 3 + [pl.BlockSpec(w.shape, lambda j, s: (0, 0)) for w in w_shapes]),
        input_output_aliases={n_in + k: k for k in range(n_alias)},
        compiler_params=pltpu.CompilerParams(dimension_semantics=("arbitrary",), vmem_limit_bytes=60 * 2 ** 20),
        cost_estimate=pl.CostEstimate(flops=20 * 2 ** 20 * 40, bytes_accessed=40 * 2 ** 20, transcendentals=2 ** 20),
    )(info, *args)


def fwd_kernel(has_alias, split, *refs):
    x_ref, wu, wd = refs[0], refs[1], refs[1 + split]
    o_ref, w1s, w2s, sem = refs[2 + split + has_alias:]
    per_dev = DROWS if split else 2 * DROWS
    i = pl.program_id(0)
    CH = DROWS
    n_ch = FF // CH

    def copies(c):
        out = []
        for d in range(8):
            src = wu.at[pl.ds(per_dev * d + (c // 2) * ROWS, ROWS), pl.ds((c % 2) * CH, CH)]
            out.append(pltpu.make_async_copy(src, w1s.at[pl.ds(d * ROWS, ROWS), pl.ds(c * CH, CH)], sem.at[0, c]))
        out.append(pltpu.make_async_copy(wd.at[pl.ds(per_dev * c + per_dev - DROWS, CH), :], w2s.at[pl.ds(c * CH, CH), :], sem.at[1, c]))
        return out

    def run(wait):
        x = x_ref[...].reshape(TM, D)
        acc = None
        for c in range(n_ch):
            if wait:
                for cp in copies(c):
                    cp.wait()
            cs = pl.ds(c * CH, CH)
            a = gelu(dot(x, w1s[:, cs], 1, 0)).astype(BF16)
            part = dot(a, w2s[cs, :], 1, 0)
            acc = part if acc is None else acc + part
        o_ref[...] = (x.astype(F32) + acc).astype(BF16).reshape(o_ref.shape)

    @pl.when(i == 0)
    def _():
        for c in range(n_ch):
            for cp in copies(c):
                cp.start()
        run(True)

    @pl.when(i > 0)
    def _():
        run(False)


def fwd_call(stage, layer, x, w, y_prev):
    if layer == 0:
        x_spec = pl.BlockSpec((1, 1, TM, D), lambda i: (stage, 0, i, 0))
        out_shape = jax.ShapeDtypeStruct((TOK, D), BF16)
        o_spec = pl.BlockSpec((TM, D), lambda i: (i, 0))
    else:
        x_spec = pl.BlockSpec((TM, D), lambda i: (i, 0))
        out_shape = jax.ShapeDtypeStruct((2, 1, TOK, D), BF16)
        o_spec = pl.BlockSpec((1, 1, TM, D), lambda i: (stage, 0, i, 0))
    split = len(w) - 1
    args = [x, *w]
    specs = [x_spec] + [ANY] * len(w)
    aliases = {}
    if y_prev is not None:
        args.append(y_prev)
        specs.append(ANY)
        aliases = {2 + split: 0}
    return pl.pallas_call(
        functools.partial(fwd_kernel, len(aliases), split),
        out_shape=out_shape,
        grid_spec=pltpu.PrefetchScalarGridSpec(
            num_scalar_prefetch=0, grid=(NB,), in_specs=specs, out_specs=o_spec,
            scratch_shapes=[pltpu.VMEM((D, FF), BF16), pltpu.VMEM((FF, D), BF16), pltpu.SemaphoreType.DMA((2, FF // DROWS))]),
        input_output_aliases=aliases,
        compiler_params=pltpu.CompilerParams(dimension_semantics=("arbitrary",), vmem_limit_bytes=60 * 2 ** 20),
        cost_estimate=pl.CostEstimate(flops=4 * TOK * D * FF, bytes_accessed=26 * 2 ** 20, transcendentals=TOK * FF),
    )(*args)


SEQ = ("bwd_010", "bwd_011", "bwd_110", "adam_01", "dx_01", "bwd_111", "bwd_000", "dx_11", "adam_11", "bwd_001", "bwd_100", "adam_00", "bwd_101", "adam_10", "fwd_00", "fwd_01", "fwd_10", "fwd_11")


def solution(mesh):
    tok_spec = P(None, 'fsdp')
    layer_spec = P(None, None, 'fsdp')
    n_dev = mesh.shape['fsdp']

    def swap(a, r):
        return lax.ppermute(a, 'fsdp', [(d, d ^ r) for d in range(n_dev)])

    def gather(a):
        return lax.all_gather(a, 'fsdp', axis=0, tiled=True)

    def device_step(x_saved, grad_out, x_next, w_up, w_down, acc_up, acc_down, master_up, master_down, moment1_up, moment1_down, moment2_up, moment2_down):
        me = lax.axis_index('fsdp').astype(jnp.int32)
        info = me.reshape(1)

        g_par = swap(grad_out, 1)
        x_par = swap(x_saved, 1)
        base = (x_saved, x_par, grad_out, g_par, w_up, w_down)

        down5 = lambda a: a.reshape(2, 2, HALVES, BW, D)
        states = (acc_up, master_up, moment1_up, moment2_up, down5(acc_down), down5(master_down), down5(moment1_down), down5(moment2_down))

        recv = {}
        dx = {}
        dh = {}
        outs6 = ()
        full = {}
        hid = {}
        y = None

        for name in SEQ:
            s, l = int(name.split("_")[1][0]), int(name.split("_")[1][1])
            if name.startswith("adam"):
                split = (s, l) == (1, 1)
                res = adam_call(s, l, info, recv[s, l], states, outs6, split)
                outs6 = tuple(res[:6])
                if split:
                    late = res[7]
                    full[s, l] = [gather(res[6])]
                else:
                    full[s, l] = [gather(res[6])]
                if (s, l) == (1, 0):
                    full[1, 1].append(gather(lax.optimization_barrier((late, res[6]))[0]))
                continue
            if name.startswith("fwd"):
                if l == 0:
                    hid[s] = fwd_call(s, 0, x_next, full[s, 0], None)
                else:
                    y = fwd_call(s, 1, hid[s], full[s, 1], y)
                continue
            if name.startswith("dx"):
                own, par = dx_call(s, l, info, dh[s, 0], dh[s, 1], w_up)
                dx[s] = ((own, swap(par, 1)), (par, swap(own, 1)))
                continue
            half = int(name[6])
            if name == "bwd_010":
                outs = bwd_call(s, l, half, 1, "swap", info, (x_saved, grad_out, w_up, w_down))
                dh[s, half] = tuple(outs[8:10])
                landed = (x_saved, outs[10], grad_out, outs[11], w_up, w_down)
            elif l == 0:
                outs = bwd_call(s, l, half, 3, "all", info, base, *dx[s])
            else:
                outs = bwd_call(s, l, half, 1, "all", info, landed if name == "bwd_011" else base)
                dh[s, half] = tuple(outs[8:])
            msgs = [outs[0], outs[4], outs[1], outs[5], outs[2], outs[6], outs[3], outs[7]]
            recv.setdefault((s, l), []).append([msgs[0]] + [swap(msgs[r], r) for r in range(1, 8)])

        up4 = lambda a: a.reshape(2, 2, DROWS, D)
        return (outs6[0], up4(outs6[3]), outs6[1], up4(outs6[4]), outs6[2], up4(outs6[5]), y)

    return jax.shard_map(device_step, mesh=mesh, in_specs=(layer_spec, tok_spec, tok_spec, P(), P()) + (layer_spec,) * 8, out_specs=(layer_spec,) * 6 + (tok_spec,), check_vma=False)
```

```python
import functools
import math

import jax
import jax.numpy as jnp
from jax import lax
from jax.experimental import pallas as pl
from jax.experimental.pallas import tpu as pltpu
from jax.sharding import PartitionSpec as P


LEARN_RATE = 0.005
BETA_ONE = 0.9
BETA_TWO = 0.95
ADAM_EPS = 1e-8
WEIGHT_DECAY = 0.1
MICROBATCHES = 2
ADAM_STEP = 2
CORR_ONE = 1.0 - BETA_ONE ** ADAM_STEP
CORR_TWO = 1.0 - BETA_TWO ** ADAM_STEP
GELU_C = math.sqrt(2.0 / math.pi)
GELU_K = 0.044715

D = 1024
FF = 4096
TOK = 2048
TM = 512
NB = TOK // TM
HALVES = 2
FC = FF // 2 // HALVES
BW = FC // 4
ROWS = D // 8
DROWS = FF // 8

F32 = jnp.float32
BF16 = jnp.bfloat16

ANY = pl.BlockSpec(memory_space=pl.ANY)


def dot(a, b, ca, cb):
    return lax.dot_general(a, b, (((ca,), (cb,)), ((), ())), preferred_element_type=F32)


def gelu_pair(h):
    hh = h * h
    t = jnp.tanh(h * (GELU_C + (GELU_C * GELU_K) * hh))
    cdf = 0.5 * t + 0.5
    grad = cdf + h * ((0.5 - 0.5 * (t * t)) * (GELU_C + (3.0 * GELU_C * GELU_K) * hh))
    return h * cdf, grad


def gelu(h):
    t = jnp.tanh(h * (GELU_C + (GELU_C * GELU_K) * (h * h)))
    return h * (0.5 * t + 0.5)


def flip(v, mask):
    total = 0
    for b in range(3):
        bit = lax.rem(lax.div(v, 2 ** b), 2)
        total = total + 2 ** b * (1 - bit if (mask >> b) & 1 else bit)
    return total


def bwd_kernel(stage, layer, half, mode, part, *refs):
    it = iter(refs)
    take = lambda k: [next(it) for _ in range(k)]
    info = next(it) if part == "all" else None
    if part == "all":
        xo, xp, do, dp, w_up, w_down = take(6)
    else:
        xo, do, w_up, w_down = take(4)
    n_extra = {1: 0, 3: 2}[mode]
    extra_own, extra_par = take(n_extra), take(n_extra)
    outs_even, outs_odd = take(4), take(4)
    if mode != 3:
        dho, dhp = take(2)
    if part == "swap":
        xp, dp = take(2)
    xb, db, w1s, w2s, acc1, acc2, act, dhs, insem, wsem = take(10)
    eb, esem = take(2) if n_extra else (None, None)
    outsem = next(it) if mode != 3 else None
    if part == "swap":
        send_sem, recv_sem = take(2)
    i = pl.program_id(0)
    n = 2 * NB
    slot = lax.rem(i, 2)
    me = info[0] if part == "all" else lax.axis_index('fsdp')
    core = lax.rem(me, 2)
    chip = lax.div(me, 2)
    partner = flip(me, 1)

    def in_copies(own, j, slot):
        rows = pl.ds(pl.multiple_of(j * TM, TM), TM)
        xs, ds, es = (xo, do, extra_own) if own else (xp, dp, extra_par)
        xs = xs.at[rows] if len(xs.shape) == 2 else xs.at[stage, layer, 0, rows]
        ds = ds.at[rows] if len(ds.shape) == 2 else ds.at[stage, 0, rows]
        out = [pltpu.make_async_copy(xs, xb.at[slot], insem.at[0, slot]),
               pltpu.make_async_copy(ds, db.at[slot], insem.at[1, slot])]
        for k, e in enumerate(es):
            out.append(pltpu.make_async_copy(e.at[rows], eb.at[k, slot], esem.at[k, slot]))
        return out

    def fetch(j, slot):
        @pl.when(j < NB)
        def _():
            for c in in_copies(True, j, slot):
                c.start()

        @pl.when(j >= NB)
        def _():
            for c in in_copies(False, j - NB, slot):
                c.start()

    def w_copies():
        out = []
        for j in range(4):
            f0 = pl.multiple_of(j * 1024 + core * 512 + half * BW, BW)
            out.append(pltpu.make_async_copy(w_up.at[stage, layer, :, pl.ds(f0, BW)], w1s.at[:, pl.ds(j * BW, BW)], wsem.at[0, j]))
            out.append(pltpu.make_async_copy(w_down.at[stage, layer, pl.ds(f0, BW), :], w2s.at[pl.ds(j * BW, BW), :], wsem.at[1, j]))
        return out

    def swap_copies():
        pairs = ((xo.at[stage, layer, 0], xp), (do.at[stage, 0], dp))
        return [pltpu.make_async_remote_copy(src_ref=a, dst_ref=b, send_sem=send_sem.at[k], recv_sem=recv_sem.at[k], device_id=(partner,), device_id_type=pl.DeviceIdType.MESH)
                for k, (a, b) in enumerate(pairs)]

    @pl.when(i == 0)
    def _():
        fetch(0, 0)
        for c in w_copies():
            c.start()
        if part == "swap":
            barrier = pltpu.get_barrier_semaphore()
            pl.semaphore_signal(barrier, inc=1, device_id=(partner,), device_id_type=pl.DeviceIdType.MESH)
            pl.semaphore_wait(barrier, 1)
            for c in swap_copies():
                c.start()
        acc1[...] = jnp.zeros_like(acc1)
        acc2[...] = jnp.zeros_like(acc2)
        for c in w_copies():
            c.wait()

    if part == "swap":
        @pl.when(i == NB - 1)
        def _():
            for c in swap_copies():
                c.wait()

    @pl.when(i + 1 < n)
    def _():
        fetch(i + 1, 1 - slot)

    for c in in_copies(True, 0, slot):
        c.wait()

    def dh_copy(own, j, slot):
        rows = pl.ds(pl.multiple_of(j * TM, TM), TM)
        return pltpu.make_async_copy(dhs.at[slot], (dho if own else dhp).at[rows], outsem.at[slot])

    if mode != 3:
        @pl.when(i >= 2)
        def _():
            dh_copy(True, 0, slot).wait()

    CH = 256
    n_ch = FC // CH
    x = xb[slot]
    dy = db[slot]
    if mode == 3:
        dy = (dy.astype(F32) + (eb[0, slot] + eb[1, slot])).astype(BF16)

    def front(c):
        cs = slice(c * CH, (c + 1) * CH)
        h = dot(x, w1s[:, cs], 1, 0)
        da = dot(dy, w2s[cs, :], 1, 1)
        g, grad = gelu_pair(h)
        act[:, cs] = g.astype(BF16)
        dhs[slot, :, cs] = (da * grad).astype(BF16)

    def back(c):
        cs = slice(c * CH, (c + 1) * CH)
        acc1[:, cs] += dot(x, dhs[slot, :, cs], 0, 0)
        acc2[cs, :] += dot(act[:, cs], dy, 0, 0)

    for c in range(n_ch):
        front(c)
    for c in range(n_ch):
        back(c)
    if mode != 3:
        @pl.when(i < NB)
        def _():
            dh_copy(True, i, slot).start()

        @pl.when(i >= NB)
        def _():
            dh_copy(False, i - NB, slot).start()

    @pl.when(i == n - 1)
    def _():
        for q in range(4):
            dev = flip(me, 2 * q)
            oc = flip(chip, q)
            outs_even[q][0:ROWS, :] = acc1[pl.ds(pl.multiple_of(dev * ROWS, ROWS), ROWS), :].astype(BF16)
            outs_even[q][ROWS:ROWS + BW, :] = acc2[pl.ds(pl.multiple_of(oc * BW, BW), BW), :].astype(BF16)
            dev = flip(me, 2 * q + 1)
            outs_odd[q][...] = acc1[pl.ds(pl.multiple_of(dev * ROWS, ROWS), ROWS), :].astype(BF16)
        if mode != 3:
            dh_copy(True, 0, 0).wait()
            dh_copy(True, 0, 1).wait()


def bwd_call(stage, layer, half, mode, part, info, base_args, extra_own=(), extra_par=()):
    out_shape = [jax.ShapeDtypeStruct((ROWS + BW, FC), BF16)] * 4 + [jax.ShapeDtypeStruct((ROWS, FC), BF16)] * 4
    out_specs = [pl.BlockSpec((ROWS + BW, FC), lambda *_: (0, 0))] * 4 + [pl.BlockSpec((ROWS, FC), lambda *_: (0, 0))] * 4
    scratch = [
        pltpu.VMEM((2, TM, D), BF16), pltpu.VMEM((2, TM, D), BF16),
        pltpu.VMEM((D, FC), BF16), pltpu.VMEM((FC, D), BF16),
        pltpu.VMEM((D, FC), F32), pltpu.VMEM((FC, D), F32),
        pltpu.VMEM((TM, FC), BF16), pltpu.VMEM((2, TM, FC), BF16),
        pltpu.SemaphoreType.DMA((2, 2)), pltpu.SemaphoreType.DMA((2, 4)),
    ]
    args = list(base_args) + list(extra_own) + list(extra_par)
    n_extra = len(extra_own)
    if n_extra:
        scratch += [pltpu.VMEM((n_extra, 2, TM, D), F32), pltpu.SemaphoreType.DMA((n_extra, 2))]
    if mode != 3:
        out_shape += [jax.ShapeDtypeStruct((TOK, FC), BF16)] * 2
        out_specs += [ANY] * 2
        scratch += [pltpu.SemaphoreType.DMA((2,))]
    params = dict(dimension_semantics=("arbitrary",), vmem_limit_bytes=63 * 2 ** 20)
    if part == "swap":
        out_shape += [jax.ShapeDtypeStruct((TOK, D), BF16)] * 2
        out_specs += [ANY] * 2
        scratch += [pltpu.SemaphoreType.DMA((2,)), pltpu.SemaphoreType.DMA((2,))]
        params.update(collective_id=0, has_side_effects=True)
    call = pl.pallas_call(
        functools.partial(bwd_kernel, stage, layer, half, mode, part),
        out_shape=out_shape,
        grid_spec=pltpu.PrefetchScalarGridSpec(
            num_scalar_prefetch=int(part == "all"), grid=(2 * NB,), in_specs=[ANY] * len(args), out_specs=out_specs, scratch_shapes=scratch),
        compiler_params=pltpu.CompilerParams(**params),
        cost_estimate=pl.CostEstimate(flops=16 * TOK * D * FC, bytes_accessed=40 * 2 ** 20, transcendentals=2 * TOK * FC),
    )
    return call(*args) if part == "swap" else call(info, *args)


def dx_kernel(stage, layer, info, h0o, h0p, h1o, h1p, w_up, dxo, dxp, dhb, w1s, dxb, insem, wsem, outsem):
    i = pl.program_id(0)
    n = 2 * NB
    slot = lax.rem(i, 2)
    core = lax.rem(info[0], 2)

    def in_copies(own, j, slot):
        rows = pl.ds(pl.multiple_of(j * TM, TM), TM)
        pair = (h0o, h1o) if own else (h0p, h1p)
        return [pltpu.make_async_copy(a.at[rows], dhb.at[slot, :, pl.ds(k * FC, FC)], insem.at[k, slot]) for k, a in enumerate(pair)]

    def fetch(j, slot):
        @pl.when(j < NB)
        def _():
            for c in in_copies(False, j, slot):
                c.start()

        @pl.when(j >= NB)
        def _():
            for c in in_copies(True, j - NB, slot):
                c.start()

    def w_copies():
        out = []
        for half in range(HALVES):
            for j in range(4):
                f0 = pl.multiple_of(j * 1024 + core * 512 + half * BW, BW)
                out.append(pltpu.make_async_copy(w_up.at[stage, layer, :, pl.ds(f0, BW)], w1s.at[:, pl.ds(half * FC + j * BW, BW)], wsem.at[half, j]))
        return out

    def out_copy(own, j, slot):
        rows = pl.ds(pl.multiple_of(j * TM, TM), TM)
        return pltpu.make_async_copy(dxb.at[slot], (dxo if own else dxp).at[rows], outsem.at[slot])

    @pl.when(i == 0)
    def _():
        fetch(0, 0)
        for c in w_copies():
            c.start()
        for c in w_copies():
            c.wait()

    @pl.when(i + 1 < n)
    def _():
        fetch(i + 1, 1 - slot)

    for c in in_copies(True, 0, slot):
        c.wait()

    @pl.when(i >= 2)
    def _():
        out_copy(True, 0, slot).wait()

    dxb[slot] = dot(dhb[slot], w1s[...], 1, 1)

    @pl.when(i < NB)
    def _():
        out_copy(False, i, slot).start()

    @pl.when(i >= NB)
    def _():
        out_copy(True, i - NB, slot).start()

    @pl.when(i == n - 1)
    def _():
        out_copy(True, 0, 0).wait()
        out_copy(True, 0, 1).wait()


def dx_call(stage, layer, info, dh0, dh1, w_up):
    args = [dh0[0], dh0[1], dh1[0], dh1[1], w_up]
    return pl.pallas_call(
        functools.partial(dx_kernel, stage, layer),
        out_shape=[jax.ShapeDtypeStruct((TOK, D), F32)] * 2,
        grid_spec=pltpu.PrefetchScalarGridSpec(
            num_scalar_prefetch=1, grid=(2 * NB,), in_specs=[ANY] * 5, out_specs=[ANY] * 2,
            scratch_shapes=[pltpu.VMEM((2, TM, HALVES * FC), BF16), pltpu.VMEM((D, HALVES * FC), BF16), pltpu.VMEM((2, TM, D), F32),
                            pltpu.SemaphoreType.DMA((2, 2)), pltpu.SemaphoreType.DMA((2, 4)), pltpu.SemaphoreType.DMA((2,))]),
        compiler_params=pltpu.CompilerParams(dimension_semantics=("arbitrary",), vmem_limit_bytes=63 * 2 ** 20),
        cost_estimate=pl.CostEstimate(flops=4 * TOK * D * HALVES * FC, bytes_accessed=38 * 2 ** 20, transcendentals=0),
    )(info, *args)


def adam(grad_new, acc, master, m1, m2):
    g = (acc + grad_new) / MICROBATCHES
    m1 = BETA_ONE * m1 + (1.0 - BETA_ONE) * g
    m2 = BETA_TWO * m2 + (1.0 - BETA_TWO) * g * g
    step_dir = (m1 * (1.0 / CORR_ONE)) / (jnp.sqrt(m2 * (1.0 / CORR_TWO)) + ADAM_EPS)
    master = master - LEARN_RATE * (step_dir + WEIGHT_DECAY * master)
    return master, m1, m2


def adam_kernel(n_alias, split, info, *refs):
    up = refs[:16]
    down = refs[16:24]
    au, mu, m1u, m2u, ad, md, m1d, m2d = refs[24:32]
    omu, om1u, om2u, omd, om1d, om2d = refs[32 + n_alias:38 + n_alias]
    w_up_out, w_down_out = refs[38 + n_alias], refs[-1]
    down0 = 0 if split else DROWS
    core = lax.rem(info[0], 2)
    j = pl.program_id(0)
    up_rows = pl.ds(pl.multiple_of(j * ROWS, ROWS), ROWS)
    for half in range(HALVES):
        for g in range(2):
            total = None
            for q in range(4):
                v = up[half * 8 + 2 * q + g][...].astype(F32)
                total = v if total is None else total + v
            col = jnp.bitwise_xor(core, g) * 512 + half * BW
            cs = pl.ds(pl.multiple_of(col, BW), BW)
            new = adam(total, au[0, 0, :, cs], mu[0, 0, :, cs], m1u[0, 0, :, cs], m2u[0, 0, :, cs])
            omu[0, 0, :, cs] = new[0]
            om1u[0, 0, :, cs] = new[1]
            om2u[0, 0, :, cs] = new[2]
            w_up_out[up_rows, cs] = new[0].astype(BF16)
        total = None
        for q in range(4):
            v = down[half * 4 + q][...].astype(F32)
            total = v if total is None else total + v
        new = adam(total, ad[0, 0, half], md[0, 0, half], m1d[0, 0, half], m2d[0, 0, half])
        omd[0, 0, half] = new[0]
        om1d[0, 0, half] = new[1]
        om2d[0, 0, half] = new[2]
        w_down_out[pl.ds(pl.multiple_of(down0 + half * BW + j * (BW // 4), BW // 4), BW // 4), :] = new[0].astype(BF16)


def adam_call(stage, layer, info, recv, states, prev, split):
    nj = 4
    dr = BW // nj
    up_spec = pl.BlockSpec((ROWS, BW), lambda j, s: (0, j))
    down_spec = pl.BlockSpec((dr, D), lambda j, s: (ROWS // dr + j, 0))
    st_up = pl.BlockSpec((1, 1, ROWS, FF // nj), lambda j, s: (stage, layer, 0, j))
    st_down = pl.BlockSpec((1, 1, HALVES, dr, D), lambda j, s: (stage, layer, 0, j, 0))
    args, specs = [], []
    for half in range(HALVES):
        for r in range(8):
            args.append(recv[half][r])
            specs.append(up_spec)
    for half in range(HALVES):
        for q in range(4):
            args.append(recv[half][2 * q])
            specs.append(down_spec)
    args += list(states)
    specs += [st_up] * 4 + [st_down] * 4
    n_alias = len(prev)
    args += list(prev)
    specs += [ANY] * n_alias
    up_shape = jax.ShapeDtypeStruct(states[0].shape, F32)
    down_shape = jax.ShapeDtypeStruct(states[4].shape, F32)
    n_in = 1 + len(args) - n_alias
    w_shapes = [jax.ShapeDtypeStruct((DROWS, D), BF16)] * 2 if split else [jax.ShapeDtypeStruct((2 * DROWS, D), BF16)]
    return pl.pallas_call(
        functools.partial(adam_kernel, n_alias, split),
        out_shape=[up_shape] * 3 + [down_shape] * 3 + w_shapes,
        grid_spec=pltpu.PrefetchScalarGridSpec(
            num_scalar_prefetch=1, grid=(nj,), in_specs=specs,
            out_specs=[st_up] * 3 + [st_down] * 3 + [pl.BlockSpec(w.shape, lambda j, s: (0, 0)) for w in w_shapes]),
        input_output_aliases={n_in + k: k for k in range(n_alias)},
        compiler_params=pltpu.CompilerParams(dimension_semantics=("arbitrary",), vmem_limit_bytes=63 * 2 ** 20),
        cost_estimate=pl.CostEstimate(flops=20 * 2 ** 20 * 40, bytes_accessed=40 * 2 ** 20, transcendentals=2 ** 20),
    )(info, *args)


def fwd_kernel(has_alias, split, *refs):
    x_ref, wu, wd = refs[0], refs[1], refs[1 + split]
    o_ref, w1s, w2s, sem = refs[2 + split + has_alias:]
    per_dev = DROWS if split else 2 * DROWS
    i = pl.program_id(0)
    CH = DROWS
    n_ch = FF // CH

    def copies(c):
        out = []
        for d in range(8):
            src = wu.at[pl.ds(per_dev * d + (c // 2) * ROWS, ROWS), pl.ds((c % 2) * CH, CH)]
            out.append(pltpu.make_async_copy(src, w1s.at[pl.ds(d * ROWS, ROWS), pl.ds(c * CH, CH)], sem.at[0, c]))
        out.append(pltpu.make_async_copy(wd.at[pl.ds(per_dev * c + per_dev - DROWS, CH), :], w2s.at[pl.ds(c * CH, CH), :], sem.at[1, c]))
        return out

    def run(wait):
        x = x_ref[...].reshape(TM, D)
        acc = None
        for c in range(n_ch):
            if wait:
                for cp in copies(c):
                    cp.wait()
            cs = pl.ds(c * CH, CH)
            a = gelu(dot(x, w1s[:, cs], 1, 0)).astype(BF16)
            part = dot(a, w2s[cs, :], 1, 0)
            acc = part if acc is None else acc + part
        o_ref[...] = (x.astype(F32) + acc).astype(BF16).reshape(o_ref.shape)

    @pl.when(i == 0)
    def _():
        for c in range(n_ch):
            for cp in copies(c):
                cp.start()
        run(True)

    @pl.when(i > 0)
    def _():
        run(False)


def fwd_call(stage, layer, x, w, y_prev):
    if layer == 0:
        x_spec = pl.BlockSpec((1, 1, TM, D), lambda i: (stage, 0, i, 0))
        out_shape = jax.ShapeDtypeStruct((TOK, D), BF16)
        o_spec = pl.BlockSpec((TM, D), lambda i: (i, 0))
    else:
        x_spec = pl.BlockSpec((TM, D), lambda i: (i, 0))
        out_shape = jax.ShapeDtypeStruct((2, 1, TOK, D), BF16)
        o_spec = pl.BlockSpec((1, 1, TM, D), lambda i: (stage, 0, i, 0))
    split = len(w) - 1
    args = [x, *w]
    specs = [x_spec] + [ANY] * len(w)
    aliases = {}
    if y_prev is not None:
        args.append(y_prev)
        specs.append(ANY)
        aliases = {2 + split: 0}
    return pl.pallas_call(
        functools.partial(fwd_kernel, len(aliases), split),
        out_shape=out_shape,
        grid_spec=pltpu.PrefetchScalarGridSpec(
            num_scalar_prefetch=0, grid=(NB,), in_specs=specs, out_specs=o_spec,
            scratch_shapes=[pltpu.VMEM((D, FF), BF16), pltpu.VMEM((FF, D), BF16), pltpu.SemaphoreType.DMA((2, FF // DROWS))]),
        input_output_aliases=aliases,
        compiler_params=pltpu.CompilerParams(dimension_semantics=("arbitrary",), vmem_limit_bytes=63 * 2 ** 20),
        cost_estimate=pl.CostEstimate(flops=4 * TOK * D * FF, bytes_accessed=26 * 2 ** 20, transcendentals=TOK * FF),
    )(*args)


SEQ = ("bwd_010", "bwd_011", "bwd_110", "adam_01", "dx_01", "bwd_111", "bwd_000", "dx_11", "adam_11", "bwd_001", "bwd_100", "adam_00", "bwd_101", "adam_10", "fwd_00", "fwd_01", "fwd_10", "fwd_11")


def solution(mesh):
    tok_spec = P(None, 'fsdp')
    layer_spec = P(None, None, 'fsdp')
    n_dev = mesh.shape['fsdp']

    def swap(a, r):
        return lax.ppermute(a, 'fsdp', [(d, d ^ r) for d in range(n_dev)])

    def gather(a):
        return lax.all_gather(a, 'fsdp', axis=0, tiled=True)

    def device_step(x_saved, grad_out, x_next, w_up, w_down, acc_up, acc_down, master_up, master_down, moment1_up, moment1_down, moment2_up, moment2_down):
        me = lax.axis_index('fsdp').astype(jnp.int32)
        info = me.reshape(1)

        g_par = swap(grad_out, 1)
        x_par = swap(x_saved, 1)
        base = (x_saved, x_par, grad_out, g_par, w_up, w_down)

        down5 = lambda a: a.reshape(2, 2, HALVES, BW, D)
        states = (acc_up, master_up, moment1_up, moment2_up, down5(acc_down), down5(master_down), down5(moment1_down), down5(moment2_down))

        recv = {}
        dx = {}
        dh = {}
        outs6 = ()
        full = {}
        hid = {}
        y = None

        for name in SEQ:
            s, l = int(name.split("_")[1][0]), int(name.split("_")[1][1])
            if name.startswith("adam"):
                split = (s, l) == (1, 1)
                res = adam_call(s, l, info, recv[s, l], states, outs6, split)
                outs6 = tuple(res[:6])
                if split:
                    late = res[7]
                    full[s, l] = [gather(res[6])]
                else:
                    full[s, l] = [gather(res[6])]
                if (s, l) == (1, 0):
                    full[1, 1].append(gather(lax.optimization_barrier((late, res[6]))[0]))
                continue
            if name.startswith("fwd"):
                if l == 0:
                    hid[s] = fwd_call(s, 0, x_next, full[s, 0], None)
                else:
                    y = fwd_call(s, 1, hid[s], full[s, 1], y)
                continue
            if name.startswith("dx"):
                own, par = dx_call(s, l, info, dh[s, 0], dh[s, 1], w_up)
                dx[s] = ((own, swap(par, 1)), (par, swap(own, 1)))
                continue
            half = int(name[6])
            if name == "bwd_010":
                outs = bwd_call(s, l, half, 1, "swap", info, (x_saved, grad_out, w_up, w_down))
                dh[s, half] = tuple(outs[8:10])
                landed = (x_saved, outs[10], grad_out, outs[11], w_up, w_down)
            elif l == 0:
                outs = bwd_call(s, l, half, 3, "all", info, base, *dx[s])
            else:
                outs = bwd_call(s, l, half, 1, "all", info, landed if name == "bwd_011" else base)
                dh[s, half] = tuple(outs[8:])
            msgs = [outs[0], outs[4], outs[1], outs[5], outs[2], outs[6], outs[3], outs[7]]
            recv.setdefault((s, l), []).append([msgs[0]] + [swap(msgs[r], r) for r in range(1, 8)])

        up4 = lambda a: a.reshape(2, 2, DROWS, D)
        return (outs6[0], up4(outs6[3]), outs6[1], up4(outs6[4]), outs6[2], up4(outs6[5]), y)

    return jax.shard_map(device_step, mesh=mesh, in_specs=(layer_spec, tok_spec, tok_spec, P(), P()) + (layer_spec,) * 8, out_specs=(layer_spec,) * 6 + (tok_spec,), check_vma=False)
```
